32 devices in a mesh: dom: 8 (over y, x, core), slab: 4 (over z).
Axes of the slice: x: 2, y: 2, z: 4, core: 2. Of those that a mesh axis runs over, the one named last changes fastest.
Arguments:
- features: bfloat16 [4096, 128], P(('dom', 'slab')), may hold values from -6 to 6
- cotangent: bfloat16 [4096, 128], P(('dom', 'slab')), may hold values from -6 to 6
- positions: float32 [3, 4096], P(None, ('dom', 'slab')), may hold values from 0 to 1, as said below
- neighbours: int32 [16, 4096], P(None, ('dom', 'slab')), may hold values from 0 to 191
- counts: int32 [4096], P(('dom', 'slab')), may hold values from 4 to 16, as said below
- k_index: int32 [3, 2048], replicated, may hold values from -8 to 8, as said below
- k_filter: float32 [2048, 128], replicated, may hold values from -0.125 to 0.125
- w_radial: bfloat16 [16, 128], replicated, may hold values from -1.5 to 1.5
- w_out: bfloat16 [128, 128], replicated, may hold values from -0.5 to 0.5
Outputs:
- d_features: float32 [4096, 128], P(('dom', 'slab'))
- d_positions: float32 [3, 4096], P(None, ('dom', 'slab'))
- d_filter: float32 [2048, 128], P(('dom', 'slab'))
- d_radial: float32 [16, 128], replicated
- d_out: float32 [128, 128], replicated
The draws below stay inside these ranges and needn't reach their ends.
Inputs may be any that keep to these rules, and one draw needn't show every extreme that they name: Atoms of domain (a, b) have positions[0] in [a / 8, (a + 1) / 8) and positions[1] in [b / 4, (b + 1) / 4). `neighbours`: entries index the domain's ghost buffer: its own 128 atoms, then 4 groups of 16 ghost atoms as the steps define. Slot s of atom i is live when s < counts[i]; the first atom of every domain uses all 16 slots. `k_index`: the 2048 vectors (columns) are distinct and non-zero, and no vector's negative is among them.
All inputs are finite; a program needn't handle non-finite values.
Results may differ from the reference program's by a relative error of at most 0.0054.
Values may be sent and summed in bfloat16 or wider, within the bound.
No kernel may reach another device: no remote copies, remote signals or barrier semaphores. Data moves between devices by JAX's collectives and lax.ppermute only.
A program may use at most 64 MiB of HBM per device.

```python
import math
import jax
import jax.numpy as jnp
from jax import lax

A_DEV = 128
NB = 16
C = 128
K = 2048
H = 128
R = 16
GH = 16
ATOMS = 4096
N_DOM = 8
N_SLAB = 4


def draw_positions(key, part):
    uniform_draw = jax.random.uniform(key, (3, ATOMS), jnp.float32)
    blocks = jnp.arange(ATOMS, dtype=jnp.int32) // A_DEV
    first_cell = (blocks // N_SLAB).astype(jnp.float32)
    second_cell = (blocks % N_SLAB).astype(jnp.float32)
    return jnp.stack([(first_cell + uniform_draw[0]) / N_DOM, (second_cell + uniform_draw[1]) / N_SLAB, uniform_draw[2]])


def draw_counts(key, part):
    drawn = jax.random.randint(key, (ATOMS,), NB // 4, NB + 1)
    leading = jnp.arange(ATOMS, dtype=jnp.int32) % A_DEV == 0
    return jnp.where(leading, NB, drawn).astype(jnp.int32)


def draw_k_index(key, part):
    side_len = 17
    cube_cells = side_len * side_len * side_len
    shuffled = jax.random.permutation(jax.random.fold_in(key, 7), jnp.arange(cube_cells, dtype=jnp.int32))
    first_idx = shuffled // (side_len * side_len) - 8
    second_idx = shuffled // side_len % side_len - 8
    third_idx = shuffled % side_len - 8
    upper_half = (first_idx > 0) | (first_idx == 0) & (second_idx > 0) | (first_idx == 0) & (second_idx == 0) & (third_idx > 0)
    ranking = jnp.argsort(jnp.where(upper_half, 0, 1).astype(jnp.int32), stable=True)
    chosen = ranking[:K]
    return jnp.stack([first_idx[chosen], second_idx[chosen], third_idx[chosen]]).astype(jnp.int32)


def with_ends(array, key, least, high):
    longest = array.shape.index(max(array.shape))
    spots = []
    for shift in (0, 1):
        where = [jax.random.randint(jax.random.fold_in(key, axis), (), 0, length) for axis, length in enumerate(array.shape)]
        where[longest] = (where[longest] + shift) % array.shape[longest]
        spots.append(tuple(where))
    return array.at[spots[0]].set(least).at[spots[1]].set(high)


def steps_of(rng, extent, pieces, smallest, largest):
    loudness = 1.0
    for axis_at, shards_of in pieces:
        draws = jax.random.uniform(jax.random.fold_in(jax.random.fold_in(rng, 6), axis_at), (shards_of,), jnp.float32, smallest / len(pieces), largest / len(pieces))
        loudness = loudness * jnp.repeat(jnp.exp(draws), extent[axis_at] // shards_of).reshape((-1,) + (1,) * (len(extent) - 1 - axis_at))
    return loudness


def bell_draw(stream_key, shape, width, reach, cuts=(), kind=jnp.bfloat16):
    values = width * jax.random.normal(stream_key, shape, jnp.float32)
    if cuts:
        values = values * steps_of(stream_key, shape, cuts, -0.22, 0.18)
    return jnp.clip(values, -reach, reach).astype(kind)


def setup_inputs(seed: int = 0) -> dict:
    seeds = jax.random.split(jax.random.key(seed), 10)
    return {
        "features": bell_draw(seeds[0], (ATOMS, C), 1.0, 6.0, ((0, 32),)),
        "cotangent": bell_draw(seeds[1], (ATOMS, C), 1.0, 6.0, ((0, 32),)),
        "positions": draw_positions(jax.random.fold_in(seeds[9], 71), 0),
        "neighbours": with_ends(jax.random.randint(seeds[3], (NB, ATOMS), 0, A_DEV + 4 * GH), jax.random.fold_in(seeds[3], 1), 0, (A_DEV + 4 * GH) - 1).astype(jnp.int32),
        "counts": draw_counts(jax.random.fold_in(seeds[9], 71), 0),
        "k_index": draw_k_index(jax.random.fold_in(seeds[9], 71), 0),
        "k_filter": bell_draw(seeds[6], (K, C), K ** -0.5, 0.125, (), jnp.float32),
        "w_radial": bell_draw(seeds[7], (R, H), R ** -0.5, 1.5),
        "w_out": bell_draw(seeds[8], (H, C), H ** -0.5, 0.5),
    }


TWO_PI = 2.0 * math.pi
HIGHEST = lax.Precision.HIGHEST

def phases(positions, k_vectors):
    phase_arg = TWO_PI * (positions[0][:, None] * k_vectors[0][None, :] + positions[1][:, None] * k_vectors[1][None, :] + positions[2][:, None] * k_vectors[2][None, :])
    return (jnp.cos(phase_arg), jnp.sin(phase_arg))

def contract_rows(first_op, second_op):
    return lax.dot_general(first_op, second_op, (((0,), (0,)), ((), ())), preferred_element_type=jnp.float32)

def contract_cols(first_op, second_op):
    return lax.dot_general(first_op, second_op, (((1,), (1,)), ((), ())), preferred_element_type=jnp.float32)

def structure_terms(features, cotangent, positions, k_vectors):
    cosine, sine_val = phases(positions, k_vectors)
    cos_half = cosine.astype(jnp.bfloat16)
    sin_half = sine_val.astype(jnp.bfloat16)
    return (contract_rows(cos_half, features), contract_rows(sin_half, features), contract_rows(cos_half, cotangent), contract_rows(sin_half, cotangent))

def long_backward(features, cotangent, positions, k_vectors, shares, pos_unit):
    fs_re, fs_im, fg_re, fg_im = shares
    cosine, sine_val = phases(positions, k_vectors)
    cos_half = cosine.astype(jnp.bfloat16)
    sin_half = sine_val.astype(jnp.bfloat16)
    d_feat = jnp.dot(cos_half, fg_re, preferred_element_type=jnp.float32) + jnp.dot(sin_half, fg_im, preferred_element_type=jnp.float32)
    along_re = contract_cols(cotangent, fs_re) + contract_cols(features, fg_re)
    along_im = contract_cols(cotangent, fs_im) + contract_cols(features, fg_im)
    weight = cosine * along_im - sine_val * along_re
    d_pos = pos_unit * lax.dot_general(k_vectors, weight, (((1,), (1,)), ((), ())), precision=HIGHEST, preferred_element_type=jnp.float32)
    return (d_feat, d_pos)

def radial_rates(levels):
    steps_n = jnp.arange(levels, dtype=jnp.float32)
    return 0.5 * jnp.exp(steps_n * (math.log(16.0) / (levels - 1)))

def pair_backward(buf_feat, buf_pos, own_pos, cotangent, neighbours, counts, w_radial, w_out, rates, pos_unit):
    slots, atom_count = neighbours.shape
    buffer_rows = buf_feat.shape[0]
    flat_index = neighbours.reshape(-1)
    target_pos = jnp.take(buf_pos, flat_index, axis=1)
    source_pos = jnp.tile(own_pos, (1, slots))
    offsets = target_pos - source_pos
    chord = jnp.sin(TWO_PI * offsets)
    dist2 = lax.optimization_barrier(jnp.sum(chord * chord, axis=0))
    rbf = jnp.exp(-rates[:, None] * dist2[None, :])
    rbf_half = rbf.astype(jnp.bfloat16)
    pre_act = lax.dot_general(rbf_half, w_radial, (((0,), (0,)), ((), ())), preferred_element_type=jnp.float32)
    gate_prob = jax.nn.sigmoid(pre_act)
    act_half = (pre_act * gate_prob).astype(jnp.bfloat16)
    filt_val = jnp.dot(act_half, w_out, preferred_element_type=jnp.float32)
    live_mask = (lax.broadcasted_iota(jnp.int32, (slots, atom_count), 0) < counts[None, :]).reshape(-1).astype(jnp.float32)
    cot_rep = jnp.tile(cotangent, (slots, 1)).astype(jnp.float32)
    weight_g = (live_mask / math.sqrt(slots))[:, None] * cot_rep
    d_buf_feat = jnp.zeros((buffer_rows, cotangent.shape[1]), jnp.float32).at[flat_index].add(weight_g * filt_val)
    feat_rows = jnp.take(buf_feat, flat_index, axis=0)
    dphi = (weight_g * feat_rows).astype(jnp.bfloat16)
    pair_out = contract_rows(act_half, dphi)
    d_act = contract_cols(dphi, w_out)
    dpre = (d_act * gate_prob * (1.0 + pre_act * (1.0 - gate_prob))).astype(jnp.bfloat16)
    pair_radial = lax.dot_general(rbf_half, dpre, (((1,), (0,)), ((), ())), preferred_element_type=jnp.float32)
    d_rbf = contract_cols(w_radial, dpre)
    d_chord2 = -lax.optimization_barrier(jnp.sum(d_rbf * rates[:, None] * rbf, axis=0))
    dmove = 2.0 * pos_unit * d_chord2[None, :] * chord * jnp.cos(TWO_PI * offsets)
    d_buf_pos = jnp.zeros((3, buffer_rows), jnp.float32).at[:, flat_index].add(dmove)
    d_own_pos = -lax.optimization_barrier(jnp.sum(dmove.reshape(3, slots, atom_count), axis=1))
    return (d_buf_feat, d_buf_pos, d_own_pos, pair_radial, pair_out)

def reference(features, cotangent, positions, neighbours, counts, k_index, k_filter, w_radial, w_out):
    devices = N_DOM * N_SLAB
    scale_norm = 1.0 / math.sqrt(ATOMS)
    pos_unit = 1.0 / math.sqrt(K)
    k_vectors = k_index.astype(jnp.float32)
    feat_blocks = features.reshape(devices, A_DEV, C)
    cot_blocks = cotangent.reshape(devices, A_DEV, C)
    pos_blocks = positions.reshape(3, devices, A_DEV).transpose(1, 0, 2)

    def add_terms(totals, blocks):
        partials = structure_terms(blocks[0], blocks[1], blocks[2], k_vectors)
        return (tuple((first_op + second_op for first_op, second_op in zip(totals, partials))), None)
    zeros_kc = jnp.zeros((K, C), jnp.float32)
    summed, _ = lax.scan(add_terms, (zeros_kc, zeros_kc, zeros_kc, zeros_kc), (feat_blocks, cot_blocks, pos_blocks))
    s_re, s_im, g_re, g_im = [scale_norm * value_kc for value_kc in summed]
    d_filter = s_re * g_re + s_im * g_im
    shares = tuple(((k_filter * value_kc).astype(jnp.bfloat16) for value_kc in (s_re, s_im, g_re, g_im)))

    def long_block(blocks):
        return long_backward(blocks[0], blocks[1], blocks[2], k_vectors, shares, pos_unit)
    d_long, dpos_long = lax.map(long_block, (feat_blocks, cot_blocks, pos_blocks))
    grid_feat = features.reshape(N_DOM, N_SLAB, A_DEV, C)
    grid_pos = positions.reshape(3, N_DOM, N_SLAB, A_DEV)

    def feat_face(face):
        return grid_feat[:, :, face * GH:(face + 1) * GH]

    def pos_face(face):
        return grid_pos[:, :, :, face * GH:(face + 1) * GH]
    ghost_feat = [jnp.roll(feat_face(1), 1, 0), jnp.roll(feat_face(0), -1, 0), jnp.roll(feat_face(3), 1, 1), jnp.roll(feat_face(2), -1, 1)]
    ghost_pos = [jnp.roll(pos_face(1), 1, 1), jnp.roll(pos_face(0), -1, 1), jnp.roll(pos_face(3), 1, 2), jnp.roll(pos_face(2), -1, 2)]
    buffer_rows = A_DEV + 4 * GH
    buf_feat = jnp.concatenate([grid_feat] + ghost_feat, axis=2).reshape(devices, buffer_rows, C)
    buf_pos = jnp.concatenate([grid_pos] + ghost_pos, axis=3).reshape(3, devices, buffer_rows).transpose(1, 0, 2)
    nbr_blocks = neighbours.reshape(NB, devices, A_DEV).transpose(1, 0, 2)
    count_blocks = counts.reshape(devices, A_DEV)
    rates = radial_rates(R)

    def pair_block(blocks):
        return pair_backward(blocks[0], blocks[1], blocks[2], blocks[3], blocks[4], blocks[5], w_radial, w_out, rates, pos_unit)
    d_buf_feat, d_buf_pos, d_own_pos, pair_radial, pair_out = lax.map(pair_block, (buf_feat, buf_pos, pos_blocks, cot_blocks, nbr_blocks, count_blocks))
    grid_dfeat = d_buf_feat.reshape(N_DOM, N_SLAB, buffer_rows, C)
    ghost_dfeat = [grid_dfeat[:, :, A_DEV + face * GH:A_DEV + (face + 1) * GH] for face in range(4)]
    returned = [jnp.roll(ghost_dfeat[0], -1, 0), jnp.roll(ghost_dfeat[1], 1, 0), jnp.roll(ghost_dfeat[2], -1, 1), jnp.roll(ghost_dfeat[3], 1, 1)]
    feat_return = jnp.concatenate([returned[1], returned[0], returned[3], returned[2], jnp.zeros((N_DOM, N_SLAB, A_DEV - 4 * GH, C), jnp.float32)], axis=2)
    short_feat = grid_dfeat[:, :, :A_DEV] + feat_return
    grid_dpos = d_buf_pos.transpose(1, 0, 2).reshape(3, N_DOM, N_SLAB, buffer_rows)
    ghost_dpos = [grid_dpos[:, :, :, A_DEV + face * GH:A_DEV + (face + 1) * GH] for face in range(4)]
    returned_pos = [jnp.roll(ghost_dpos[0], -1, 1), jnp.roll(ghost_dpos[1], 1, 1), jnp.roll(ghost_dpos[2], -1, 2), jnp.roll(ghost_dpos[3], 1, 2)]
    pos_return = jnp.concatenate([returned_pos[1], returned_pos[0], returned_pos[3], returned_pos[2], jnp.zeros((3, N_DOM, N_SLAB, A_DEV - 4 * GH), jnp.float32)], axis=3)
    own_moves = d_own_pos.transpose(1, 0, 2).reshape(3, N_DOM, N_SLAB, A_DEV)
    short_pos = grid_dpos[:, :, :, :A_DEV] + pos_return + own_moves
    d_features = d_long.reshape(ATOMS, C) + short_feat.reshape(ATOMS, C)
    d_positions = dpos_long.transpose(1, 0, 2).reshape(3, ATOMS) + short_pos.reshape(3, ATOMS)
    d_radial = scale_norm * lax.optimization_barrier(jnp.sum(pair_radial, axis=0))
    d_out = scale_norm * lax.optimization_barrier(jnp.sum(pair_out, axis=0))
    return (d_features, d_positions, d_filter, d_radial, d_out)
```

```python
import functools
import math

import jax
import jax.numpy as jnp
from jax import lax
from jax.experimental import pallas as pl
from jax.experimental.pallas import tpu as pltpu
from jax.sharding import PartitionSpec as P


F32 = jnp.float32
BF16 = jnp.bfloat16
POS_ROWS = 32
MAGIC = 12582912.0
SIN_POLY = (
    6.28318528028833,
    -10.335420168095697,
    5.100155056857644,
    -1.196582599540606,
    0.15531532235506335,
)
COS_POLY = (
    0.9999999532943689,
    -4.934792832496617,
    4.058411371007551,
    -1.331876617475819,
    0.21968961468319229,
)


def horner(coefs, w):
    acc = jnp.full_like(w, coefs[-1])
    for c in coefs[-2::-1]:
        acc = acc * w + c
    return acc


def turn_trig(t):
    u = t - ((t + MAGIC) - MAGIC)
    w = u * u
    twice_sin = u * horner(SIN_POLY, w)
    half_cos = horner(COS_POLY, w)
    return 1.0 - 0.5 * twice_sin * twice_sin, twice_sin * half_cos


def three_pieces(value):
    high = value.astype(BF16)
    rest = value - high.astype(F32)
    mid = rest.astype(BF16)
    low = (rest - mid.astype(F32)).astype(BF16)
    return high, mid, low


def mm(first, second, dims):
    return lax.dot_general(first, second, (dims, ((), ())), preferred_element_type=F32)


NN = ((1,), (0,))
TN = ((0,), (0,))
NT = ((1,), (1,))


def pos_of(rows):
    rows = rows.astype(F32)
    return rows[0:8] + rows[8:16] + rows[16:24]


def structure_body(atoms, n_msg, rows, k_ref, *refs):
    msgs, (s_ref, cos_ref, sin_ref) = refs[:n_msg], refs[n_msg:]
    k_total = k_ref.shape[1]
    places = jnp.concatenate([m[2 * atoms : 2 * atoms + POS_ROWS] for m in msgs], axis=1)
    values = jnp.concatenate(
        [
            jnp.concatenate([m[:atoms], m[atoms : 2 * atoms]], axis=1)
            for m in (ref[...] for ref in msgs)
        ],
        axis=0,
    )
    width = values.shape[1]
    for j in range(k_total // rows):
        span = slice(j * rows, (j + 1) * rows)
        turns = mm(k_ref[:, span], places, TN)
        cosine, sine = turn_trig(turns)
        cos_ref[span, :] = cosine
        sin_ref[span, :] = sine
        s_ref[span, :width] = mm(cosine.astype(BF16), values, NN)
        s_ref[span, width:] = mm(sine.astype(BF16), values, NN)


def structure(k_rows, msgs, atoms, channels):
    k_total = k_rows.shape[1]
    n = len(msgs)
    table = jax.ShapeDtypeStruct((k_total, n * atoms), F32)
    return pl.pallas_call(
        functools.partial(structure_body, atoms, n, min(128, k_total)),
        out_shape=(jax.ShapeDtypeStruct((k_total, 4 * channels), F32), table, table),
        compiler_params=pltpu.CompilerParams(vmem_limit_bytes=24 * 2**20),
        cost_estimate=pl.CostEstimate(
            flops=4_000_000_000, bytes_accessed=4_000_000, transcendentals=0
        ),
        name="structure",
    )(k_rows, *msgs)


def shares_body(scale, own_ref, filter_ref, *refs):
    others, (d_filter_ref, share_ref) = refs[:-2], refs[-2:]
    total = own_ref[...]
    for other in others:
        total = total + other[...].astype(F32)
    total = scale * total
    c = filter_ref.shape[1]
    s_re, g_re = total[:, :c], total[:, c : 2 * c]
    s_im, g_im = total[:, 2 * c : 3 * c], total[:, 3 * c :]
    d_filter_ref[...] = s_re * g_re + s_im * g_im
    k_filter = filter_ref[...]
    share_ref[...] = (jnp.concatenate([k_filter] * 4, axis=1) * total).astype(BF16)


def make_shares(scale, own, k_filter, others):
    rows, channels = k_filter.shape
    return pl.pallas_call(
        functools.partial(shares_body, scale),
        out_shape=(
            jax.ShapeDtypeStruct((rows, channels), F32),
            jax.ShapeDtypeStruct((rows, 4 * channels), BF16),
        ),
        compiler_params=pltpu.CompilerParams(vmem_limit_bytes=8 * 2**20),
        cost_estimate=pl.CostEstimate(
            flops=200_000_000, bytes_accessed=600_000, transcendentals=0
        ),
        name="shares",
    )(own, k_filter, *others)


def half_backward(atoms, pos_unit, msgs, k_ref, cos_ref, sin_ref, shares):
    c = shares[0].shape[1] // 4
    share = jnp.concatenate([s[...] for s in shares], axis=0)
    source = jnp.concatenate(
        [
            jnp.concatenate([m[atoms : 2 * atoms], m[:atoms]], axis=1)
            for m in (ref[...] for ref in msgs)
        ],
        axis=0,
    )
    cosine, sine = cos_ref[...], sin_ref[...]
    feat = mm(share[:, c : 2 * c], cosine.astype(BF16), TN) + mm(
        share[:, 3 * c :], sine.astype(BF16), TN
    )
    p = mm(share[:, : 2 * c], source, NT)
    q = mm(share[:, 2 * c :], source, NT)
    weight = cosine * q - sine * p
    high = weight.astype(BF16)
    low = (weight - high.astype(F32)).astype(BF16)
    k8 = k_ref[0:16, :]
    place = mm(k8, high, NN) + mm(k8, low, NN)
    return feat, pos_unit * place[0:8]


def back_first_body(atoms, n_msg, n_share, pos_unit, k_ref, cos_ref, sin_ref, *refs):
    msgs = refs[:n_msg]
    shares = refs[n_msg : n_msg + n_share]
    feat_ref, place_ref = refs[n_msg + n_share :]
    feat, place = half_backward(atoms, pos_unit, msgs, k_ref, cos_ref, sin_ref, shares)
    feat_ref[...] = feat
    place_ref[...] = place


def back_last_body(atoms, n_msg, n_share, pos_unit, k_ref, cos_ref, sin_ref, *refs):
    msgs = refs[:n_msg]
    shares = refs[n_msg : n_msg + n_share]
    feat0_ref, place0_ref, buf_ref, move_ref = refs[n_msg + n_share : n_msg + n_share + 4]
    own_feat_ref, own_place_ref, *out_refs = refs[n_msg + n_share + 4 :]
    feat, place = half_backward(atoms, pos_unit, msgs, k_ref, cos_ref, sin_ref, shares)
    feat = feat + feat0_ref[...]
    place = place + place0_ref[...]
    face = atoms // 8
    lane = lax.broadcasted_iota(jnp.int32, (8, atoms), 1)
    ghost_move = move_ref[:, atoms : 2 * atoms]
    for d in range(n_msg):
        rows = feat[:, d * atoms : (d + 1) * atoms].T
        spots = place[:, d * atoms : (d + 1) * atoms]
        if d == 0:
            own_feat_ref[...] = rows + buf_ref[:atoms]
            own_place_ref[...] = spots + move_ref[:, :atoms]
            continue
        for shift, ghost, group in ((1, 2, 3), (n_msg - 1, 3, 2)):
            if d == shift:
                part = buf_ref[atoms + ghost * face : atoms + (ghost + 1) * face]
                pieces = [rows[: group * face], rows[group * face : (group + 1) * face] + part]
                rows = jnp.concatenate(pieces + [rows[(group + 1) * face :]], axis=0)
                rolled = pltpu.roll(ghost_move, ((group - ghost) * face) % atoms, 1)
                inside = (lane >= group * face) & (lane < (group + 1) * face)
                spots = spots + jnp.where(inside, rolled, 0.0)
        out = out_refs[d - 1]
        out[:atoms, :] = rows.astype(BF16)
        high, mid, low = three_pieces(spots)
        out[atoms:, :] = jnp.concatenate([high, mid, low, jnp.zeros_like(low)], axis=0)


def back_call(body, out_shape, name, *operands):
    return pl.pallas_call(
        body,
        out_shape=out_shape,
        compiler_params=pltpu.CompilerParams(vmem_limit_bytes=24 * 2**20),
        cost_estimate=pl.CostEstimate(
            flops=3_000_000_000, bytes_accessed=4_000_000, transcendentals=0
        ),
        name=name,
    )(*operands)


def pair_body(
    atoms,
    channels,
    group,
    pos_unit,
    own_ref,
    below_d,
    above_d,
    below_s,
    above_s,
    nbr_ref,
    count_ref,
    wr_ref,
    wo_ref,
    buf_out,
    move_out,
    grad_out,
    ret0_ref,
    ret1_ref,
    buf_acc,
    mat_ref,
):
    slots = nbr_ref.shape[0]
    levels, hidden = wr_ref.shape
    face = atoms // 8
    wide = 2 * atoms
    span = group * atoms
    f32_of = lambda rows: rows.astype(F32)
    lane = lax.broadcasted_iota(jnp.int32, (POS_ROWS, atoms), 1)
    ghost = jnp.zeros((POS_ROWS, atoms), F32)
    ghosts = ((below_d, 1), (above_d, 0), (below_s, 3), (above_s, 2))
    for slot, (ref, source) in enumerate(ghosts):
        rolled = pltpu.roll(f32_of(ref[face : face + POS_ROWS]), ((slot - source) * face) % atoms, 1)
        inside = (lane >= slot * face) & (lane < (slot + 1) * face)
        ghost = jnp.where(inside, rolled, ghost)
    own_rows = own_ref[2 * atoms : 2 * atoms + POS_ROWS]
    places = jnp.concatenate([own_rows, ghost.astype(BF16)], axis=1)
    rows = [f32_of(own_ref[:atoms])] + [f32_of(ref[:face]) for ref, _ in ghosts]
    rows.append(jnp.zeros((wide - atoms - 4 * face, channels), F32))
    features_t = jnp.concatenate(rows, axis=0).T.astype(BF16)
    mat_ref[:channels, :] = features_t
    mat_ref[channels:, :] = places
    cot_t = f32_of(own_ref[atoms : 2 * atoms]).T * (1.0 / math.sqrt(slots))
    source_pos = pos_of(own_rows)
    source_pos = jnp.concatenate([source_pos] * group, axis=1)
    cot_rep = jnp.concatenate([cot_t] * group, axis=1)
    steps = lax.broadcasted_iota(jnp.int32, (levels, span), 0).astype(F32)
    rates = 0.5 * jnp.exp(steps * (math.log(16.0) / (levels - 1)))
    buffer_row = lax.broadcasted_iota(jnp.int32, (wide, span), 0)
    w_radial = wr_ref[...]
    w_out = wo_ref[...]
    buf_acc[...] = jnp.zeros_like(buf_acc)
    grad_out[...] = jnp.zeros_like(grad_out)
    move_out[...] = jnp.zeros_like(move_out)

    def step(g, carry):
        index = jnp.concatenate([nbr_ref[pl.ds(g * group + s, 1), :] for s in range(group)], axis=1)
        live = jnp.concatenate(
            [jnp.where(count_ref[...] > g * group + s, 1.0, 0.0) for s in range(group)], axis=1
        )
        picked = jnp.where(buffer_row == index, 1.0, 0.0).astype(BF16)
        taken = mm(mat_ref[...], picked, NN)
        feat = taken[:channels]
        offset = pos_of(taken[channels:]) - source_pos
        cosine, chord = turn_trig(offset)
        dist2 = jnp.sum(chord * chord, axis=0, keepdims=True)
        rbf = jnp.exp(-rates * dist2)
        rbf_h = rbf.astype(BF16)
        pre = mm(w_radial, rbf_h, TN)
        gate = jax.nn.sigmoid(pre)
        act = (pre * gate).astype(BF16)
        phi = mm(w_out, act, TN)
        weight = cot_rep * live
        message = weight * phi
        high = message.astype(BF16)
        low = (message - high.astype(F32)).astype(BF16)
        buf_acc[...] += mm(picked, high, NT) + mm(picked, low, NT)
        dphi = (weight * feat).astype(BF16)
        grad_out[levels:, :] += mm(act, dphi, NT)
        d_act = mm(w_out, dphi, NN)
        dpre = (d_act * gate * (1.0 + pre * (1.0 - gate))).astype(BF16)
        grad_out[:levels, :] += mm(rbf_h, dpre, NT)
        d_rbf = mm(w_radial, dpre, NN)
        d_chord2 = -jnp.sum(d_rbf * rates * rbf, axis=0, keepdims=True)
        dmove = (2.0 * pos_unit) * d_chord2 * chord * cosine
        pieces = jnp.concatenate([v.astype(F32) for v in three_pieces(dmove)], axis=0).astype(BF16)
        moved = mm(pieces, picked, NT)
        move_out[...] += moved[0:8] + moved[8:16] + moved[16:24]
        back = dmove[:, :atoms]
        for s in range(1, group):
            back = back + dmove[:, s * atoms : (s + 1) * atoms]
        move_out[:, :atoms] -= back
        return carry

    lax.fori_loop(0, slots // group, step, 0)
    buf_out[...] = buf_acc[: atoms + 4 * face]
    for ref, slot in ((ret0_ref, 0), (ret1_ref, 1)):
        ref[:face, :] = buf_acc[atoms + slot * face : atoms + (slot + 1) * face]
        ref[face:, :] = move_out[:, atoms:]


def pair_part(own, ghosts, neighbours, counts, w_radial, w_out, pos_unit):
    slots, atoms = neighbours.shape
    levels, hidden = w_radial.shape
    channels = w_out.shape[1]
    face = atoms // 8
    group = 4
    ret = jax.ShapeDtypeStruct((face + 8, channels), F32)
    return pl.pallas_call(
        functools.partial(pair_body, atoms, channels, group, pos_unit),
        out_shape=(
            jax.ShapeDtypeStruct((atoms + 4 * face, channels), F32),
            jax.ShapeDtypeStruct((8, 2 * atoms), F32),
            jax.ShapeDtypeStruct((levels + hidden, channels), F32),
            ret,
            ret,
        ),
        scratch_shapes=[
            pltpu.VMEM((2 * atoms, channels), F32),
            pltpu.VMEM((channels + POS_ROWS, 2 * atoms), BF16),
        ],
        compiler_params=pltpu.CompilerParams(vmem_limit_bytes=16 * 2**20),
        cost_estimate=pl.CostEstimate(
            flops=4_000_000_000, bytes_accessed=1_000_000, transcendentals=500_000
        ),
        name="pairs",
    )(own, *ghosts, neighbours, counts.reshape(1, atoms), w_radial, w_out)


def finish_body(n_msg, own_feat, own_place, ret0, ret1, *refs):
    msgs, (feat_ref, pos_ref) = refs[:n_msg], refs[n_msg:]
    atoms = own_feat.shape[0]
    face = atoms // 8
    feat = own_feat[...]
    place = own_place[...]
    for m in msgs:
        feat = feat + m[:atoms].astype(F32)
        place = place + pos_of(m[atoms : atoms + POS_ROWS])
    feat_ref[2 * face :, :] = feat[2 * face :]
    feat_ref[:face, :] = feat[:face] + ret1[:face]
    feat_ref[face : 2 * face, :] = feat[face : 2 * face] + ret0[:face]
    lane = lax.broadcasted_iota(jnp.int32, (8, atoms), 1)
    below = pltpu.roll(ret1[face : face + 8], atoms - face, 1)
    above = pltpu.roll(ret0[face : face + 8], face, 1)
    place = place + jnp.where(lane < face, below, 0.0)
    place = place + jnp.where((lane >= face) & (lane < 2 * face), above, 0.0)
    pos_ref[...] = place[0:3]


def finish(own_feat, own_place, ret0, ret1, msgs):
    atoms, channels = own_feat.shape
    return pl.pallas_call(
        functools.partial(finish_body, len(msgs)),
        out_shape=(
            jax.ShapeDtypeStruct((atoms, channels), F32),
            jax.ShapeDtypeStruct((3, atoms), F32),
        ),
        compiler_params=pltpu.CompilerParams(vmem_limit_bytes=8 * 2**20),
        name="finish",
    )(own_feat, own_place, ret0, ret1, *msgs)


def along(block, axis, shift):
    n = lax.axis_size(axis)
    return lax.ppermute(block, axis, [((i - shift) % n, i) for i in range(n)])


def swapped(block, axis, mask):
    n = lax.axis_size(axis)
    return lax.ppermute(block, axis, [(i, i ^ mask) for i in range(n)])


def bits_of(n):
    return [1 << b for b in range(n.bit_length() - 1)]


def reordered(values, index, axis):
    n = values.shape[axis]
    for bit in bits_of(n):
        shape = values.shape[:axis] + (n // (2 * bit), 2, bit) + values.shape[axis + 1 :]
        split = values.reshape(shape)
        turned = jnp.flip(split, axis + 1)
        values = jnp.where((index & bit) > 0, turned, split).reshape(values.shape)
    return values


def rounded(value):
    return lax.reduce_precision(value, 8, 7)


def shards(features, cotangent, positions, neighbours, counts, k_index, k_filter, w_radial, w_out):
    atoms, channels = features.shape
    n_dom, n_slab = lax.axis_size("dom"), lax.axis_size("slab")
    devices = n_dom * n_slab
    chips = n_dom // 2
    scale = 1.0 / math.sqrt(atoms * devices)
    k_total = k_index.shape[1]
    pos_unit = 1.0 / math.sqrt(k_total)
    block = k_total // devices
    face = atoms // 8
    dom, slab = lax.axis_index("dom"), lax.axis_index("slab")

    high = rounded(positions)
    mid = rounded(positions - high)
    low = positions - high - mid
    gap = jnp.zeros((5, atoms), F32)
    last = jnp.zeros((POS_ROWS - 24, atoms), F32)
    places = jnp.concatenate([high, gap, mid, gap, low, gap, last], axis=0).astype(BF16)
    own = jnp.concatenate([features, cotangent, places], axis=0)
    msgs = [own] + [along(own, "slab", d) for d in range(1, n_slab)]

    def face_of(g):
        return jnp.concatenate([features[g * face : (g + 1) * face], places], axis=0)

    ghosts = [
        along(face_of(1), "dom", 1),
        along(face_of(0), "dom", -1),
        along(face_of(3), "slab", 1),
        along(face_of(2), "slab", -1),
    ]

    k_own = lax.dynamic_index_in_dim(k_index.reshape(3, n_dom, n_slab, block), slab, 2, False)
    k_own = reordered(k_own, dom, 1).reshape(3, chips, 2, block).transpose(0, 2, 1, 3)
    k_rows = jnp.pad(k_own.reshape(3, n_dom * block), ((0, 5), (0, 0))).astype(BF16)
    k_rows = jnp.concatenate([k_rows, k_rows, k_rows, jnp.zeros_like(k_rows)], axis=0)
    half = chips * block
    k_here, k_there = k_rows[:, :half], k_rows[:, half:]
    filter_rows = lax.dynamic_slice_in_dim(k_filter, (dom * n_slab + slab) * block, block, 0)

    buf, moves, grads, ret0, ret1 = pair_part(
        own, ghosts, neighbours, counts, w_radial, w_out, pos_unit
    )

    s_there, cos_there, sin_there = structure(k_there, msgs, atoms, channels)
    s_sent = swapped(s_there, "dom", 1)
    s_here, cos_here, sin_here = structure(k_here, msgs, atoms, channels)
    s_sum = s_here + s_sent
    pieces = [s_sum[s * block : (s + 1) * block].astype(BF16) for s in range(1, chips)]
    arrived = [swapped(piece, "dom", 2 * s) for s, piece in enumerate(pieces, 1)]
    d_filter, share = make_shares(scale, s_sum[:block], filter_rows, arrived)

    shares_here = [share] + [swapped(share, "dom", 2 * s) for s in range(1, chips)]
    shares_there = [swapped(value, "dom", 1) for value in shares_here]

    ret_above = along(ret0, "dom", -1)
    ret_below = along(ret1, "dom", 1)
    for axis, n in (("dom", n_dom), ("slab", n_slab)):
        for bit in bits_of(n):
            grads = grads + swapped(grads, axis, bit)

    n_msg, n_share = len(msgs), len(shares_here)
    feat_0, place_0 = back_call(
        functools.partial(back_first_body, atoms, n_msg, n_share, pos_unit),
        (
            jax.ShapeDtypeStruct((channels, n_msg * atoms), F32),
            jax.ShapeDtypeStruct((8, n_msg * atoms), F32),
        ),
        "back_first",
        k_here,
        cos_here,
        sin_here,
        *msgs,
        *shares_here,
    )
    message = jax.ShapeDtypeStruct((atoms + POS_ROWS, channels), BF16)
    own_feat, own_place, *partials = back_call(
        functools.partial(back_last_body, atoms, n_msg, n_share, pos_unit),
        (
            jax.ShapeDtypeStruct((atoms, channels), F32),
            jax.ShapeDtypeStruct((8, atoms), F32),
        )
        + (message,) * (n_msg - 1),
        "back_last",
        k_there,
        cos_there,
        sin_there,
        *msgs,
        *shares_there,
        feat_0,
        place_0,
        buf,
        moves,
    )
    returned = [along(part, "slab", -d) for d, part in enumerate(partials, 1)]
    d_features, d_positions = finish(own_feat, own_place, ret_above, ret_below, returned)
    levels = w_radial.shape[0]
    return (d_features, d_positions, d_filter, scale * grads[:levels], scale * grads[levels:])


def solution(mesh):
    in_specs = (
        P(("dom", "slab"), None),
        P(("dom", "slab"), None),
        P(None, ("dom", "slab")),
        P(None, ("dom", "slab")),
        P(("dom", "slab")),
        P(),
        P(),
        P(),
        P(),
    )
    out_specs = (
        P(("dom", "slab"), None),
        P(None, ("dom", "slab")),
        P(("dom", "slab"), None),
        P(),
        P(),
    )
    return jax.shard_map(shards, mesh=mesh, in_specs=in_specs, out_specs=out_specs, check_vma=False)
```

```python
import functools
import math

import jax
import jax.numpy as jnp
from jax import lax
from jax.experimental import pallas as pl
from jax.experimental.pallas import tpu as pltpu
from jax.sharding import PartitionSpec as P


F32 = jnp.float32
BF16 = jnp.bfloat16
GROUP = 16
POS_ROWS = 32
MAGIC = 12582912.0
SIN_POLY = (
    6.28318528028833,
    -10.335420168095697,
    5.100155056857644,
    -1.196582599540606,
    0.15531532235506335,
)
COS_POLY = (
    0.9999999532943689,
    -4.934792832496617,
    4.058411371007551,
    -1.331876617475819,
    0.21968961468319229,
)


def horner(coefs, w):
    acc = jnp.full_like(w, coefs[-1])
    for c in coefs[-2::-1]:
        acc = acc * w + c
    return acc


def turn_trig(t):
    u = t - ((t + MAGIC) - MAGIC)
    w = u * u
    twice_sin = u * horner(SIN_POLY, w)
    half_cos = horner(COS_POLY, w)
    return 1.0 - 0.5 * twice_sin * twice_sin, twice_sin * half_cos


def three_pieces(value):
    high = value.astype(BF16)
    rest = value - high.astype(F32)
    mid = rest.astype(BF16)
    low = (rest - mid.astype(F32)).astype(BF16)
    return high, mid, low


def mm(first, second, dims):
    return lax.dot_general(first, second, (dims, ((), ())), preferred_element_type=F32)


NN = ((1,), (0,))
TN = ((0,), (0,))
NT = ((1,), (1,))


def place_rows(positions):
    n = positions.shape[1]
    filled = jnp.concatenate([positions, jnp.zeros((5, n), F32)], axis=0)
    pieces = [v.astype(F32) for v in three_pieces(filled)]
    pieces.append(jnp.zeros((POS_ROWS - 24, n), F32))
    return jnp.concatenate(pieces, axis=0).astype(BF16)


def pos_of(rows):
    rows = rows.astype(F32)
    return rows[0:8] + rows[8:16] + rows[16:24]


def pack_body(feat_hbm, cot_hbm, pos_hbm, own_ref, face_ref, pos_ref, sems):
    atoms = feat_hbm.shape[0]
    faces = 2 * (atoms // 8)
    copies = [
        pltpu.make_async_copy(pos_hbm, pos_ref, sems.at[0]),
        pltpu.make_async_copy(feat_hbm, own_ref.at[pl.ds(0, atoms)], sems.at[1]),
        pltpu.make_async_copy(cot_hbm, own_ref.at[pl.ds(atoms, atoms)], sems.at[2]),
    ]
    for copy in copies:
        copy.start()
    copies[0].wait()
    places = place_rows(pos_ref[...])
    own_ref[2 * atoms :, :] = places
    face_ref[faces:, :] = places
    copies[1].wait()
    face_ref[:faces, :] = own_ref[:faces]
    copies[2].wait()


def pack(features, cotangent, positions):
    atoms, channels = features.shape
    return pl.pallas_call(
        pack_body,
        out_shape=(
            jax.ShapeDtypeStruct((2 * atoms + POS_ROWS, channels), BF16),
            jax.ShapeDtypeStruct((2 * (atoms // 8) + POS_ROWS, channels), BF16),
        ),
        in_specs=[pl.BlockSpec(memory_space=pl.ANY)] * 3,
        scratch_shapes=[pltpu.VMEM((3, atoms), F32), pltpu.SemaphoreType.DMA((3,))],
        name="pack",
    )(features, cotangent, positions)


def structure_rows(atoms, k_ref, msgs, cos_ref, sin_ref):
    k_total = k_ref.shape[1]
    places = jnp.concatenate([m[2 * atoms :] for m in msgs], axis=1)
    values = jnp.concatenate(
        [jnp.concatenate([m[:atoms], m[atoms : 2 * atoms]], axis=1) for m in msgs], axis=0
    )
    rows = min(128, k_total)
    for j in range(k_total // rows):
        span = slice(j * rows, (j + 1) * rows)
        cosine, sine = turn_trig(mm(k_ref[:, span], places, TN))
        cos_ref[span, :] = cosine
        sin_ref[span, :] = sine
        yield span, mm(cosine.astype(BF16), values, NN), mm(sine.astype(BF16), values, NN)


def structure_first_body(atoms, n_msg, k_ref, *refs):
    msgs, (s_ref, cos_ref, sin_ref) = refs[:n_msg], refs[n_msg:]
    for span, re, im in structure_rows(atoms, k_ref, msgs, cos_ref, sin_ref):
        s_ref[span, : re.shape[1]] = re
        s_ref[span, re.shape[1] :] = im


def structure_last_body(atoms, n_msg, k_ref, *refs):
    msgs, (s_ref, cos_ref, sin_ref, own_ref, *piece_refs) = refs[:n_msg], refs[n_msg:]
    block = own_ref.shape[0]
    for span, re, im in structure_rows(atoms, k_ref, msgs, cos_ref, sin_ref):
        width = re.shape[1]
        re = re + s_ref[span, :width]
        im = im + s_ref[span, width:]
        for j in range((span.stop - span.start) // block):
            at = span.start // block + j
            part = slice(j * block, (j + 1) * block)
            if at == 0:
                own_ref[:, :width] = re[part]
                own_ref[:, width:] = im[part]
            else:
                piece_refs[at - 1][:, :width] = re[part].astype(BF16)
                piece_refs[at - 1][:, width:] = im[part].astype(BF16)


def structure(k_rows, msgs, atoms, channels, partial=None, chips=1):
    k_total = k_rows.shape[1]
    n = len(msgs)
    table = jax.ShapeDtypeStruct((k_total, n * atoms), F32)
    if partial is None:
        body, name, extra = structure_first_body, "structure_first", ()
        shapes = (jax.ShapeDtypeStruct((k_total, 4 * channels), F32), table, table)
    else:
        body, name, extra = structure_last_body, "structure_last", (partial,)
        block = k_total // chips
        own = jax.ShapeDtypeStruct((block, 4 * channels), F32)
        piece = jax.ShapeDtypeStruct((block, 4 * channels), BF16)
        shapes = (table, table, own) + (piece,) * (chips - 1)
    return pl.pallas_call(
        functools.partial(body, atoms, n),
        out_shape=shapes,
        compiler_params=pltpu.CompilerParams(vmem_limit_bytes=8 * 2**20),
        cost_estimate=pl.CostEstimate(
            flops=4_000_000_000, bytes_accessed=4_000_000, transcendentals=0
        ),
        name=name,
    )(k_rows, *msgs, *extra)


def extra_rows(grad_rows, face):
    return -(-max(-(-grad_rows // 3), face + 16) // 16) * 16


def shares_body(scale, own_ref, filter_ref, extra_ref, *refs):
    others, (total_ref, share_ref) = refs[:-2], refs[-2:]
    total = own_ref[...]
    for other in others:
        total = total + other[...].astype(F32)
    total = scale * total
    total_ref[...] = total
    extra = extra_ref.shape[0]
    share_ref[:extra, :] = extra_ref[...]
    share_ref[extra:, :] = (jnp.concatenate([filter_ref[...]] * 4, axis=1) * total).astype(BF16)


def make_shares(scale, own, k_filter, extra, others):
    return pl.pallas_call(
        functools.partial(shares_body, scale),
        out_shape=(
            jax.ShapeDtypeStruct(own.shape, F32),
            jax.ShapeDtypeStruct((extra.shape[0] + own.shape[0], own.shape[1]), BF16),
        ),
        compiler_params=pltpu.CompilerParams(vmem_limit_bytes=8 * 2**20),
        cost_estimate=pl.CostEstimate(
            flops=200_000_000, bytes_accessed=600_000, transcendentals=0
        ),
        name="shares",
    )(own, k_filter, extra, *others)


def half_backward(atoms, pos_unit, msgs, k_ref, cos_ref, sin_ref, shares, extra):
    c = shares[0].shape[1] // 4
    share = jnp.concatenate([s[extra:] for s in shares], axis=0)
    source = jnp.concatenate(
        [
            jnp.concatenate([m[atoms : 2 * atoms], m[:atoms]], axis=1)
            for m in (ref[...] for ref in msgs)
        ],
        axis=0,
    )
    cosine, sine = cos_ref[...], sin_ref[...]
    feat = mm(share[:, c : 2 * c], cosine.astype(BF16), TN) + mm(
        share[:, 3 * c :], sine.astype(BF16), TN
    )
    p = mm(share[:, : 2 * c], source, NT)
    q = mm(share[:, 2 * c :], source, NT)
    weight = cosine * q - sine * p
    high = weight.astype(BF16)
    low = (weight - high.astype(F32)).astype(BF16)
    k8 = k_ref[0:16, :]
    place = mm(k8, high, NN) + mm(k8, low, NN)
    return feat, pos_unit * place[0:8]


def group_rows(value, face, atoms, group):
    c = value.shape[1]
    above, below = group * face, atoms - (group + 1) * face
    pieces = [jnp.zeros((above, c), F32)] if above else []
    return jnp.concatenate(pieces + [value, jnp.zeros((below, c), F32)], axis=0)


def group_lanes(value, face, source, group):
    atoms = value.shape[1]
    lane = lax.broadcasted_iota(jnp.int32, value.shape, 1)
    turned = pltpu.roll(value, ((group - source) * face) % atoms, 1)
    return jnp.where((lane >= group * face) & (lane < (group + 1) * face), turned, 0.0)


def back_other_body(atoms, n_msg, n_share, pos_unit, extra, where_ref, k_ref, cos_ref, sin_ref, *refs):
    msgs, refs = refs[:n_msg], refs[n_msg:]
    shares, refs = refs[:n_share], refs[n_share:]
    buf_ref, move_ref, grad0_ref, sum_ref = refs
    c = buf_ref.shape[1]
    face = atoms // 8
    grad = grad0_ref[...]
    passed = jnp.zeros((face, c), F32)
    passed_moves = jnp.zeros((8, atoms), F32)
    for j, ref in enumerate(shares):
        if j:
            parts = [ref[:extra, i * c : (i + 1) * c].astype(F32) for i in range(3)]
            grad = grad + jnp.concatenate(parts, axis=0)[: grad.shape[0]]
        backs = ref[: face + 16, 3 * c :].astype(F32)
        sel = jnp.where(where_ref[0] == j, 1.0, 0.0)
        passed = passed + sel * backs[:face]
        tile = backs[face : face + 8]
        passed_moves = passed_moves + sel * (tile + pltpu.roll(tile, 5, 0) + backs[face + 8 :])
    even = jnp.where(where_ref[1] == 0, 1.0, 0.0)
    odd = 1.0 - even
    ghost_0, ghost_1 = buf_ref[atoms : atoms + face], buf_ref[atoms + face : atoms + 2 * face]
    rows_0 = even * ghost_1 + odd * passed
    rows_1 = even * passed + odd * ghost_0
    ours = move_ref[:, atoms:]
    moves = group_lanes(even * ours + odd * passed_moves, face, 1, 0) + group_lanes(
        even * passed_moves + odd * ours, face, 0, 1
    )
    feat, place = half_backward(atoms, pos_unit, msgs, k_ref, cos_ref, sin_ref, shares, extra)
    for d in range(n_msg):
        rows = feat[:, d * atoms : (d + 1) * atoms].T
        spots = place[:, d * atoms : (d + 1) * atoms]
        if d == 0:
            top = jnp.concatenate([rows_0, rows_1], axis=0)
            rows = jnp.concatenate([rows[: 2 * face] + top, rows[2 * face :]], axis=0)
            spots = spots + moves
        sum_ref[d * atoms : (d + 1) * atoms, :] = rows
        first = n_msg * atoms + d * 8
        sum_ref[first : first + 8, :] = spots
    sum_ref[n_msg * (atoms + 8) :, :] = grad


def back_own_body(atoms, n_msg, n_share, pos_unit, extra, k_ref, cos_ref, sin_ref, *refs):
    msgs, refs = refs[:n_msg], refs[n_msg:]
    shares, refs = refs[:n_share], refs[n_share:]
    buf_ref, move_ref, sum_ref = refs
    c = buf_ref.shape[1]
    face = atoms // 8
    feat, place = half_backward(atoms, pos_unit, msgs, k_ref, cos_ref, sin_ref, shares, extra)
    ghost_move = move_ref[:, atoms:]
    for d in range(n_msg):
        rows = feat[:, d * atoms : (d + 1) * atoms].T
        spots = place[:, d * atoms : (d + 1) * atoms]
        if d == 0:
            rows = rows + buf_ref[:atoms]
            spots = spots + move_ref[:, :atoms]
        for shift, ghost, group in ((1, 2, 3), (n_msg - 1, 3, 2)):
            if d == shift:
                part = buf_ref[atoms + ghost * face : atoms + (ghost + 1) * face]
                rows = rows + group_rows(part, face, atoms, group)
                spots = spots + group_lanes(ghost_move, face, ghost, group)
        sum_ref[d * atoms : (d + 1) * atoms, :] = rows
        first = n_msg * atoms + d * 8
        sum_ref[first : first + 8, :] = spots


def join_body(atoms, n_msg, here_ref, there_ref, sent_ref, own_ref, *out_refs):
    tail = n_msg * (atoms + 8)
    grad = sent_ref[tail:] + there_ref[tail:]
    own_ref[atoms + 8 :, :] = grad
    grad = grad.astype(BF16)
    for d in range(n_msg):
        span = slice(d * atoms, (d + 1) * atoms)
        spot = slice(n_msg * atoms + d * 8, n_msg * atoms + d * 8 + 8)
        rows = here_ref[span] + sent_ref[span]
        spots = here_ref[spot] + sent_ref[spot]
        if d == 0:
            own_ref[:atoms, :] = rows
            own_ref[atoms : atoms + 8, :] = spots
            continue
        out = out_refs[d - 1]
        out[:atoms, :] = rows.astype(BF16)
        high, mid, low = three_pieces(spots)
        places = jnp.concatenate([high, mid, low, jnp.zeros_like(low)], axis=0)
        out[atoms : atoms + POS_ROWS, :] = places
        out[atoms + POS_ROWS :, :] = grad


def back_call(body, out_shape, name, *operands):
    specs = [pl.BlockSpec(memory_space=pltpu.VMEM)] * len(operands)
    if operands[0].dtype == jnp.int32:
        specs[0] = pl.BlockSpec(memory_space=pltpu.SMEM)
    return pl.pallas_call(
        body,
        out_shape=out_shape,
        in_specs=specs,
        compiler_params=pltpu.CompilerParams(vmem_limit_bytes=8 * 2**20),
        cost_estimate=pl.CostEstimate(
            flops=3_000_000_000, bytes_accessed=4_000_000, transcendentals=0
        ),
        name=name,
    )(*operands)


def pair_body(
    atoms,
    channels,
    group,
    pos_unit,
    where_ref,
    own_ref,
    flip_ref,
    cross_ref,
    below_ref,
    above_ref,
    nbr_ref,
    count_ref,
    wr_ref,
    wo_ref,
    buf_out,
    move_out,
    grad_out,
    extra_ref,
    buf_acc,
    mat_ref,
):
    slots = nbr_ref.shape[0]
    levels, hidden = wr_ref.shape
    face = atoms // 8
    wide = 2 * atoms
    span = group * atoms
    f32_of = lambda rows: rows.astype(F32)
    even = jnp.where(where_ref[1] == 0, 1.0, 0.0)
    odd = 1.0 - even
    cross = f32_of(cross_ref[...])
    flip_faces, flip_spots = f32_of(flip_ref[: 2 * face]), f32_of(flip_ref[2 * atoms :])
    below = odd * flip_faces + even * cross[: 2 * face]
    above = even * flip_faces + odd * cross[: 2 * face]
    ghosts = (
        (below[face:], odd * flip_spots + even * cross[2 * face :], 1),
        (above[:face], even * flip_spots + odd * cross[2 * face :], 0),
        (f32_of(below_ref[3 * face : 4 * face]), f32_of(below_ref[2 * atoms :]), 3),
        (f32_of(above_ref[2 * face : 3 * face]), f32_of(above_ref[2 * atoms :]), 2),
    )
    lane = lax.broadcasted_iota(jnp.int32, (POS_ROWS, atoms), 1)
    ghost = jnp.zeros((POS_ROWS, atoms), F32)
    for slot, (_, spot, source) in enumerate(ghosts):
        turned = pltpu.roll(spot, ((slot - source) * face) % atoms, 1)
        inside = (lane >= slot * face) & (lane < (slot + 1) * face)
        ghost = jnp.where(inside, turned, ghost)
    own_rows = own_ref[2 * atoms :]
    places = jnp.concatenate([own_rows, ghost.astype(BF16)], axis=1)
    rows = [f32_of(own_ref[:atoms])] + [g[0] for g in ghosts]
    rows.append(jnp.zeros((wide - atoms - 4 * face, channels), F32))
    features_t = jnp.concatenate(rows, axis=0).T.astype(BF16)
    mat_ref[:channels, :] = features_t
    mat_ref[channels:, :] = places
    cot_t = f32_of(own_ref[atoms : 2 * atoms]).T * (1.0 / math.sqrt(slots))
    source_pos = pos_of(own_rows)
    source_pos = jnp.concatenate([source_pos] * group, axis=1)
    cot_rep = jnp.concatenate([cot_t] * group, axis=1)
    steps = lax.broadcasted_iota(jnp.int32, (levels, span), 0).astype(F32)
    rates = 0.5 * jnp.exp(steps * (math.log(16.0) / (levels - 1)))
    buffer_row = lax.broadcasted_iota(jnp.int32, (wide, span), 0)
    w_radial = wr_ref[...]
    w_out = wo_ref[...]
    buf_acc[...] = jnp.zeros_like(buf_acc)
    grad_out[...] = jnp.zeros_like(grad_out)
    move_out[...] = jnp.zeros_like(move_out)

    def step(g, carry):
        index = jnp.concatenate([nbr_ref[pl.ds(g * group + s, 1), :] for s in range(group)], axis=1)
        live = jnp.concatenate(
            [jnp.where(count_ref[...] > g * group + s, 1.0, 0.0) for s in range(group)], axis=1
        )
        picked = jnp.where(buffer_row == index, 1.0, 0.0).astype(BF16)
        taken = mm(mat_ref[...], picked, NN)
        feat = taken[:channels]
        offset = pos_of(taken[channels:]) - source_pos
        cosine, chord = turn_trig(offset)
        dist2 = jnp.sum(chord * chord, axis=0, keepdims=True)
        rbf = jnp.exp(-rates * dist2)
        rbf_h = rbf.astype(BF16)
        pre = mm(w_radial, rbf_h, TN)
        gate = jax.nn.sigmoid(pre)
        act = (pre * gate).astype(BF16)
        phi = mm(w_out, act, TN)
        weight = cot_rep * live
        message = weight * phi
        high = message.astype(BF16)
        low = (message - high.astype(F32)).astype(BF16)
        buf_acc[...] += mm(picked, high, NT) + mm(picked, low, NT)
        dphi = (weight * feat).astype(BF16)
        grad_out[levels:, :] += mm(act, dphi, NT)
        d_act = mm(w_out, dphi, NN)
        dpre = (d_act * gate * (1.0 + pre * (1.0 - gate))).astype(BF16)
        grad_out[:levels, :] += mm(rbf_h, dpre, NT)
        d_rbf = mm(w_radial, dpre, NN)
        d_chord2 = -jnp.sum(d_rbf * rates * rbf, axis=0, keepdims=True)
        dmove = (2.0 * pos_unit) * d_chord2 * chord * cosine
        pieces = jnp.concatenate([v.astype(F32) for v in three_pieces(dmove)], axis=0).astype(BF16)
        moved = mm(pieces, picked, NT)
        move_out[...] += moved[0:8] + moved[8:16] + moved[16:24]
        back = dmove[:, :atoms]
        for s in range(1, group):
            back = back + dmove[:, s * atoms : (s + 1) * atoms]
        move_out[:, :atoms] -= back
        return carry

    lax.fori_loop(0, slots // group, step, 0)
    buf_out[...] = buf_acc[: atoms + 4 * face]
    extra = extra_ref.shape[0]
    for j in range(3):
        part = grad_out[j * extra : min((j + 1) * extra, levels + hidden)]
        extra_ref[: part.shape[0], j * channels : (j + 1) * channels] = part.astype(BF16)
    high, mid, low = (f32_of(v) for v in three_pieces(move_out[:, atoms:]))
    places = jnp.concatenate([high + pltpu.roll(mid, 3, 0), low], axis=0)
    group_0, group_1 = buf_acc[atoms : atoms + face], buf_acc[atoms + face : atoms + 2 * face]
    extra_ref[:face, 3 * channels :] = (even * group_0 + odd * group_1).astype(BF16)
    extra_ref[face : face + 16, 3 * channels :] = places.astype(BF16)


def pair_part(where, sources, neighbours, counts, w_radial, w_out, pos_unit):
    slots, atoms = neighbours.shape
    levels, hidden = w_radial.shape
    channels = w_out.shape[1]
    face = atoms // 8
    group = GROUP
    return pl.pallas_call(
        functools.partial(pair_body, atoms, channels, group, pos_unit),
        out_shape=(
            jax.ShapeDtypeStruct((atoms + 4 * face, channels), F32),
            jax.ShapeDtypeStruct((8, 2 * atoms), F32),
            jax.ShapeDtypeStruct((levels + hidden, channels), F32),
            jax.ShapeDtypeStruct((extra_rows(levels + hidden, face), 4 * channels), BF16),
        ),
        scratch_shapes=[
            pltpu.VMEM((2 * atoms, channels), F32),
            pltpu.VMEM((channels + POS_ROWS, 2 * atoms), BF16),
        ],
        in_specs=[pl.BlockSpec(memory_space=pltpu.SMEM)]
        + [pl.BlockSpec(memory_space=pltpu.VMEM)] * (len(sources) + 4),
        compiler_params=pltpu.CompilerParams(vmem_limit_bytes=12 * 2**20),
        cost_estimate=pl.CostEstimate(
            flops=4_000_000_000, bytes_accessed=1_000_000, transcendentals=500_000
        ),
        name="pairs",
    )(where, *sources, neighbours, counts.reshape(1, atoms), w_radial, w_out)


def finish_body(atoms, n_msg, scale, own_ref, total_ref, *refs):
    msgs, (feat_ref, pos_ref, filter_ref, radial_ref, out_ref) = refs[:n_msg], refs[n_msg:]
    feat, place, grad = own_ref[:atoms], own_ref[atoms : atoms + 8], own_ref[atoms + 8 :]
    for m in msgs:
        feat = feat + m[:atoms].astype(F32)
        place = place + pos_of(m[atoms : atoms + POS_ROWS])
        grad = grad + m[atoms + POS_ROWS :].astype(F32)
    levels = radial_ref.shape[0]
    c = feat_ref.shape[1]
    re = total_ref[:, :c] * total_ref[:, c : 2 * c]
    filter_ref[...] = re + total_ref[:, 2 * c : 3 * c] * total_ref[:, 3 * c :]
    feat_ref[...] = feat
    pos_ref[...] = place[0:3]
    radial_ref[...] = scale * grad[:levels]
    out_ref[...] = scale * grad[levels:]


def finish(scale, atoms, levels, own, total, msgs):
    channels = own.shape[1]
    return pl.pallas_call(
        functools.partial(finish_body, atoms, len(msgs), scale),
        out_shape=(
            jax.ShapeDtypeStruct((atoms, channels), F32),
            jax.ShapeDtypeStruct((3, atoms), F32),
            jax.ShapeDtypeStruct((total.shape[0], channels), F32),
            jax.ShapeDtypeStruct((levels, channels), F32),
            jax.ShapeDtypeStruct((own.shape[0] - atoms - 8 - levels, channels), F32),
        ),
        compiler_params=pltpu.CompilerParams(vmem_limit_bytes=8 * 2**20),
        name="finish",
    )(own, total, *msgs)


def along(block, axis, shift):
    n = lax.axis_size(axis)
    return lax.ppermute(block, axis, [((i - shift) % n, i) for i in range(n)])


def swapped(block, axis, mask):
    n = lax.axis_size(axis)
    return lax.ppermute(block, axis, [(i, i ^ mask) for i in range(n)])


def bits_of(n):
    return [1 << b for b in range(n.bit_length() - 1)]


def reordered(values, index, axis):
    n = values.shape[axis]
    for bit in bits_of(n):
        shape = values.shape[:axis] + (n // (2 * bit), 2, bit) + values.shape[axis + 1 :]
        split = values.reshape(shape)
        turned = jnp.flip(split, axis + 1)
        values = jnp.where((index & bit) > 0, turned, split).reshape(values.shape)
    return values


def shards(features, cotangent, positions, neighbours, counts, k_index, k_filter, w_radial, w_out):
    atoms, channels = features.shape
    n_dom, n_slab = lax.axis_size("dom"), lax.axis_size("slab")
    devices = n_dom * n_slab
    chips = n_dom // 2
    scale = 1.0 / math.sqrt(atoms * devices)
    k_total = k_index.shape[1]
    pos_unit = 1.0 / math.sqrt(k_total)
    block = k_total // devices
    dom, slab = lax.axis_index("dom"), lax.axis_index("slab")

    own, faces = pack(features, cotangent, positions)
    msgs = [own] + [along(own, "slab", d) for d in range(1, n_slab)]
    across = [(i, (i + 1 if i % 2 else i - 1) % n_dom) for i in range(n_dom)]
    cross = lax.ppermute(faces, "dom", across)
    others = [swapped(msg, "dom", 1) for msg in msgs]

    core, chip = dom & 1, dom >> 1
    k_own = k_index.reshape(3, chips, 2 * n_slab, block)
    k_own = lax.dynamic_index_in_dim(k_own, core * n_slab + slab, 2, False)
    k_own = reordered(k_own, chip, 1).reshape(3, chips * block)
    k_rows = jnp.pad(k_own, ((0, 5), (0, 0))).astype(BF16)
    k_rows = jnp.concatenate([k_rows, k_rows, k_rows, jnp.zeros_like(k_rows)], axis=0)
    filter_rows = lax.dynamic_slice_in_dim(k_filter, (dom * n_slab + slab) * block, block, 0)
    across_of = ((dom ^ 1) + jnp.where(core == 0, 1, n_dom - 1)) % n_dom
    where = jnp.stack([(across_of >> 1) ^ chip, core]).astype(jnp.int32)
    msgs, k_rows, filter_rows, where = lax.optimization_barrier(
        (msgs, k_rows, filter_rows, where)
    )

    partial, cos_own, sin_own = structure(k_rows, msgs, atoms, channels)
    cos_other, sin_other, s_own, *pieces = structure(
        k_rows, others, atoms, channels, partial, chips
    )
    arrived = [swapped(piece, "dom", 2 * s) for s, piece in enumerate(pieces, 1)]

    cross, pieces = lax.optimization_barrier((cross, pieces))
    sources = (msgs[0], others[0], cross, msgs[1], msgs[-1])
    buf, moves, grads, riders = pair_part(
        where, sources, neighbours, counts, w_radial, w_out, pos_unit
    )
    total, share = make_shares(scale, s_own, filter_rows, riders, arrived)
    shares = [share] + [swapped(share, "dom", 2 * s) for s in range(1, chips)]

    extra = share.shape[0] - block
    settings = (atoms, n_slab, len(shares), pos_unit, extra)
    rows = n_slab * (atoms + 8)
    there = back_call(
        functools.partial(back_other_body, *settings),
        jax.ShapeDtypeStruct((rows + grads.shape[0], channels), F32),
        "back_other",
        where,
        k_rows,
        cos_other,
        sin_other,
        *others,
        *shares,
        buf,
        moves,
        grads,
    )
    sent = swapped(there, "dom", 1)
    here = back_call(
        functools.partial(back_own_body, *settings),
        jax.ShapeDtypeStruct((rows, channels), F32),
        "back_own",
        k_rows,
        cos_own,
        sin_own,
        *msgs,
        *shares,
        buf,
        moves,
    )
    message = jax.ShapeDtypeStruct((atoms + POS_ROWS + grads.shape[0], channels), BF16)
    own_sum, *partials = back_call(
        functools.partial(join_body, atoms, n_slab),
        (jax.ShapeDtypeStruct((atoms + 8 + grads.shape[0], channels), F32),)
        + (message,) * (n_slab - 1),
        "join",
        here,
        there,
        sent,
    )
    returned = [along(part, "slab", -d) for d, part in enumerate(partials, 1)]
    return finish(scale, atoms, w_radial.shape[0], own_sum, total, returned)


def solution(mesh):
    in_specs = (
        P(("dom", "slab"), None),
        P(("dom", "slab"), None),
        P(None, ("dom", "slab")),
        P(None, ("dom", "slab")),
        P(("dom", "slab")),
        P(),
        P(),
        P(),
        P(),
    )
    out_specs = (
        P(("dom", "slab"), None),
        P(None, ("dom", "slab")),
        P(("dom", "slab"), None),
        P(),
        P(),
    )
    return jax.shard_map(shards, mesh=mesh, in_specs=in_specs, out_specs=out_specs, check_vma=False)
```

```python
import functools
import math

import jax
import jax.numpy as jnp
from jax import lax
from jax.experimental import pallas as pl
from jax.experimental.pallas import tpu as pltpu
from jax.sharding import PartitionSpec as P


F32 = jnp.float32
BF16 = jnp.bfloat16
GROUP = 16
POS_ROWS = 16
MAGIC = 12582912.0
SIN_POLY = (
    6.28318528028833,
    -10.335420168095697,
    5.100155056857644,
    -1.196582599540606,
    0.15531532235506335,
)
COS_POLY = (
    0.9999999532943689,
    -4.934792832496617,
    4.058411371007551,
    -1.331876617475819,
    0.21968961468319229,
)


def horner(coefs, w):
    acc = jnp.full_like(w, coefs[-1])
    for c in coefs[-2::-1]:
        acc = acc * w + c
    return acc


def turn_trig(t):
    u = t - ((t + MAGIC) - MAGIC)
    w = u * u
    twice_sin = u * horner(SIN_POLY, w)
    half_cos = horner(COS_POLY, w)
    return 1.0 - 0.5 * twice_sin * twice_sin, twice_sin * half_cos


def three_pieces(value):
    high = value.astype(BF16)
    rest = value - high.astype(F32)
    mid = rest.astype(BF16)
    low = (rest - mid.astype(F32)).astype(BF16)
    return high, mid, low


def mm(first, second, dims):
    return lax.dot_general(first, second, (dims, ((), ())), preferred_element_type=F32)


NN = ((1,), (0,))
TN = ((0,), (0,))
NT = ((1,), (1,))


def packed(value):
    high, mid, low = (piece.astype(F32) for piece in three_pieces(value))
    return (high + pltpu.roll(mid, 3, 0)).astype(BF16), low.astype(BF16)


def place_rows(positions):
    zeros = jnp.zeros((5, positions.shape[1]), F32)
    first, second = packed(jnp.concatenate([positions, zeros], axis=0))
    return jnp.concatenate([first.astype(F32), second.astype(F32)], axis=0).astype(BF16)


def pos_of(rows, pieces=3):
    rows = rows.astype(F32)
    total = rows[0:8] + pltpu.roll(rows[0:8], 5, 0)
    return total + rows[8:16] if pieces == 3 else total


def pack_body(feat_hbm, cot_hbm, pos_hbm, own_ref, face_ref, pos_ref, sems):
    atoms = feat_hbm.shape[0]
    faces = 2 * (atoms // 8)
    copies = [
        pltpu.make_async_copy(pos_hbm, pos_ref, sems.at[0]),
        pltpu.make_async_copy(feat_hbm, own_ref.at[pl.ds(0, atoms)], sems.at[1]),
        pltpu.make_async_copy(cot_hbm, own_ref.at[pl.ds(atoms, atoms)], sems.at[2]),
    ]
    for copy in copies:
        copy.start()
    copies[0].wait()
    places = place_rows(pos_ref[...])
    own_ref[2 * atoms :, :] = places
    face_ref[faces:, :] = places
    copies[1].wait()
    face_ref[:faces, :] = own_ref[:faces]
    copies[2].wait()


def pack(features, cotangent, positions):
    atoms, channels = features.shape
    return pl.pallas_call(
        pack_body,
        out_shape=(
            jax.ShapeDtypeStruct((2 * atoms + POS_ROWS, channels), BF16),
            jax.ShapeDtypeStruct((2 * (atoms // 8) + POS_ROWS, channels), BF16),
        ),
        in_specs=[pl.BlockSpec(memory_space=pl.ANY)] * 3,
        scratch_shapes=[pltpu.VMEM((3, atoms), F32), pltpu.SemaphoreType.DMA((3,))],
        name="pack",
    )(features, cotangent, positions)


def structure_body(atoms, n_msg, has_partial, block, k_ref, *refs):
    msgs, refs = refs[:n_msg], refs[n_msg:]
    partial, refs = (refs[0], refs[1:]) if has_partial else (None, refs)
    cos_refs, sin_refs, out_refs = refs[:n_msg], refs[n_msg : 2 * n_msg], refs[2 * n_msg :]
    k_total = k_ref.shape[1]
    places = jnp.concatenate([m[2 * atoms :] for m in msgs], axis=1)
    values = jnp.concatenate(
        [jnp.concatenate([m[:atoms], m[atoms : 2 * atoms]], axis=1) for m in msgs], axis=0
    )
    rows = min(128, k_total)
    for j in range(k_total // rows):
        span = slice(j * rows, (j + 1) * rows)
        cosine, sine = turn_trig(mm(k_ref[:, span], places, TN))
        for i, (cos_ref, sin_ref) in enumerate(zip(cos_refs, sin_refs)):
            cos_ref[span, :] = cosine[:, i * atoms : (i + 1) * atoms]
            sin_ref[span, :] = sine[:, i * atoms : (i + 1) * atoms]
        re, im = mm(cosine.astype(BF16), values, NN), mm(sine.astype(BF16), values, NN)
        width = re.shape[1]
        if has_partial:
            re = re + partial[span, :width]
            im = im + partial[span, width:]
        if len(out_refs) == 1:
            out_refs[0][span, :width] = re
            out_refs[0][span, width:] = im
            continue
        for at in range(span.start // block, span.stop // block):
            part = slice(at * block - span.start, (at + 1) * block - span.start)
            out_refs[at][:, :width] = re[part].astype(out_refs[at].dtype)
            out_refs[at][:, width:] = im[part].astype(out_refs[at].dtype)


def structure(k_rows, msgs, atoms, channels, partial=None, chips=1):
    k_total = k_rows.shape[1]
    n = len(msgs)
    block = k_total // chips
    tables = (jax.ShapeDtypeStruct((k_total, atoms), F32),) * (2 * n)
    sums = (jax.ShapeDtypeStruct((block, 4 * channels), F32),)
    sums += (jax.ShapeDtypeStruct((block, 4 * channels), BF16),) * (chips - 1)
    operands = (k_rows, *msgs) + (() if partial is None else (partial,))
    outs = pl.pallas_call(
        functools.partial(structure_body, atoms, n, partial is not None, block),
        out_shape=tables + sums,
        compiler_params=pltpu.CompilerParams(vmem_limit_bytes=8 * 2**20),
        cost_estimate=pl.CostEstimate(
            flops=1_000_000_000 * n, bytes_accessed=1_000_000 * n, transcendentals=0
        ),
    )(*operands)
    return outs[:n], outs[n : 2 * n], outs[2 * n :]


def extra_rows(grad_rows, face):
    return -(-max(-(-grad_rows // 3), face + 16) // 16) * 16


def shares_body(scale, own_ref, filter_ref, extra_ref, *refs):
    others, (total_ref, share_ref) = refs[:-2], refs[-2:]
    total = own_ref[...]
    for other in others:
        total = total + other[...].astype(F32)
    total = scale * total
    total_ref[...] = total
    extra = extra_ref.shape[0]
    share_ref[:extra, :] = extra_ref[...]
    share_ref[extra:, :] = (jnp.concatenate([filter_ref[...]] * 4, axis=1) * total).astype(BF16)


def make_shares(scale, own, k_filter, extra, others):
    return pl.pallas_call(
        functools.partial(shares_body, scale),
        out_shape=(
            jax.ShapeDtypeStruct(own.shape, F32),
            jax.ShapeDtypeStruct((extra.shape[0] + own.shape[0], own.shape[1]), BF16),
        ),
        compiler_params=pltpu.CompilerParams(vmem_limit_bytes=8 * 2**20),
        cost_estimate=pl.CostEstimate(
            flops=200_000_000, bytes_accessed=600_000, transcendentals=0
        ),
        name="shares",
    )(own, k_filter, extra, *others)


def half_backward(atoms, pos_unit, msgs, k_ref, cos_refs, sin_refs, shares, extra):
    c = shares[0].shape[1] // 4
    share = jnp.concatenate([s[extra:] for s in shares], axis=0)
    source = jnp.concatenate(
        [
            jnp.concatenate([m[atoms : 2 * atoms], m[:atoms]], axis=1)
            for m in (ref[...] for ref in msgs)
        ],
        axis=0,
    )
    cosine = jnp.concatenate([ref[...] for ref in cos_refs], axis=1)
    sine = jnp.concatenate([ref[...] for ref in sin_refs], axis=1)
    feat = mm(share[:, c : 2 * c], cosine.astype(BF16), TN) + mm(
        share[:, 3 * c :], sine.astype(BF16), TN
    )
    p = mm(share[:, : 2 * c], source, NT)
    q = mm(share[:, 2 * c :], source, NT)
    weight = cosine * q - sine * p
    high = weight.astype(BF16)
    low = (weight - high.astype(F32)).astype(BF16)
    k16 = k_ref[...]
    place = (mm(k16, high, NN) + mm(k16, low, NN))[0:8]
    row = lax.broadcasted_iota(jnp.int32, place.shape, 0)
    return feat, jnp.where(row < 3, pos_unit * place, 0.0)


def group_rows(value, face, atoms, group):
    c = value.shape[1]
    above, below = group * face, atoms - (group + 1) * face
    pieces = [jnp.zeros((above, c), F32)] if above else []
    return jnp.concatenate(pieces + [value, jnp.zeros((below, c), F32)], axis=0)


def group_lanes(value, face, source, group):
    atoms = value.shape[1]
    lane = lax.broadcasted_iota(jnp.int32, value.shape, 1)
    turned = pltpu.roll(value, ((group - source) * face) % atoms, 1)
    return jnp.where((lane >= group * face) & (lane < (group + 1) * face), turned, 0.0)


def back_other_body(atoms, n_msg, n_share, pos_unit, extra, where_ref, k_ref, *refs):
    cos_refs, sin_refs, msgs = refs[:n_msg], refs[n_msg : 2 * n_msg], refs[2 * n_msg : 3 * n_msg]
    refs = refs[3 * n_msg :]
    shares, refs = refs[:n_share], refs[n_share:]
    buf_ref, move_ref, grad0_ref, sum_ref = refs
    c = buf_ref.shape[1]
    face = atoms // 8
    grad = grad0_ref[...]
    passed = jnp.zeros((face, c), F32)
    passed_moves = jnp.zeros((8, atoms), F32)
    for j, ref in enumerate(shares):
        if j:
            parts = [ref[:extra, i * c : (i + 1) * c].astype(F32) for i in range(3)]
            grad = grad + jnp.concatenate(parts, axis=0)[: grad.shape[0]]
        backs = ref[: face + 16, 3 * c :].astype(F32)
        sel = where_ref[2 + j : 3 + j]
        passed = passed + sel * backs[:face]
        tile = backs[face : face + 8]
        passed_moves = passed_moves + sel * (tile + pltpu.roll(tile, 5, 0) + backs[face + 8 :])
    even, odd = where_ref[0:1], where_ref[1:2]
    ghost_0, ghost_1 = buf_ref[atoms : atoms + face], buf_ref[atoms + face : atoms + 2 * face]
    rows_0 = even * ghost_1 + odd * passed
    rows_1 = even * passed + odd * ghost_0
    ours = move_ref[:, atoms:]
    moves = group_lanes(even * ours + odd * passed_moves, face, 1, 0) + group_lanes(
        even * passed_moves + odd * ours, face, 0, 1
    )
    feat, place = half_backward(
        atoms, pos_unit, msgs, k_ref, cos_refs, sin_refs, shares, extra
    )
    for d in range(n_msg):
        rows = feat[:, d * atoms : (d + 1) * atoms].T
        spots = place[:, d * atoms : (d + 1) * atoms]
        if d == 0:
            top = jnp.concatenate([rows_0, rows_1], axis=0)
            rows = jnp.concatenate([rows[: 2 * face] + top, rows[2 * face :]], axis=0)
            spots = spots + moves
        sum_ref[d * atoms : (d + 1) * atoms, :] = rows
        first = n_msg * atoms + d * 8
        sum_ref[first : first + 8, :] = spots
    sum_ref[n_msg * (atoms + 8) :, :] = grad


def back_own_body(atoms, n_msg, n_share, pos_unit, extra, k_ref, *refs):
    cos_refs, sin_refs, msgs = refs[:n_msg], refs[n_msg : 2 * n_msg], refs[2 * n_msg : 3 * n_msg]
    refs = refs[3 * n_msg :]
    shares, refs = refs[:n_share], refs[n_share:]
    buf_ref, move_ref, sum_ref = refs
    face = atoms // 8
    feat, place = half_backward(
        atoms, pos_unit, msgs, k_ref, cos_refs, sin_refs, shares, extra
    )
    ghost_move = move_ref[:, atoms:]
    for d in range(n_msg):
        rows = feat[:, d * atoms : (d + 1) * atoms].T
        spots = place[:, d * atoms : (d + 1) * atoms]
        if d == 0:
            rows = rows + buf_ref[:atoms]
            spots = spots + move_ref[:, :atoms]
        for shift, ghost, group in ((1, 2, 3), (n_msg - 1, 3, 2)):
            if d == shift:
                part = buf_ref[atoms + ghost * face : atoms + (ghost + 1) * face]
                rows = rows + group_rows(part, face, atoms, group)
                spots = spots + group_lanes(ghost_move, face, ghost, group)
        sum_ref[d * atoms : (d + 1) * atoms, :] = rows
        first = n_msg * atoms + d * 8
        sum_ref[first : first + 8, :] = spots


def join_body(atoms, n_msg, here_ref, there_ref, sent_ref, own_ref, *out_refs):
    tail = n_msg * (atoms + 8)
    row = lax.broadcasted_iota(jnp.int32, (8, atoms), 0)
    grad = sent_ref[tail:] + there_ref[tail:]
    own_ref[atoms + 8 :, :] = grad
    grad = grad.astype(BF16)
    for d in range(n_msg):
        span = slice(d * atoms, (d + 1) * atoms)
        spot = slice(n_msg * atoms + d * 8, n_msg * atoms + d * 8 + 8)
        rows = here_ref[span] + sent_ref[span]
        spots = here_ref[spot] + sent_ref[spot]
        if d == 0:
            own_ref[:atoms, :] = rows
            own_ref[atoms : atoms + 8, :] = spots
            continue
        out = out_refs[d - 1]
        out[:atoms, :] = rows.astype(BF16)
        spots = jnp.where(row < 3, spots, 0.0)
        out[atoms : atoms + POS_ROWS, :] = jnp.concatenate(packed(spots), axis=0)
        out[atoms + POS_ROWS :, :] = grad


def back_call(body, out_shape, *operands):
    return pl.pallas_call(
        body,
        out_shape=out_shape,
        compiler_params=pltpu.CompilerParams(vmem_limit_bytes=8 * 2**20),
        cost_estimate=pl.CostEstimate(
            flops=3_000_000_000, bytes_accessed=4_000_000, transcendentals=0
        ),
    )(*operands)


def pair_body(
    atoms,
    channels,
    group,
    pos_unit,
    where_ref,
    own_ref,
    flip_ref,
    cross_ref,
    below_ref,
    above_ref,
    nbr_ref,
    count_ref,
    wr_ref,
    wo_ref,
    buf_out,
    move_out,
    grad_out,
    extra_ref,
    buf_acc,
    mat_ref,
):
    slots = nbr_ref.shape[0]
    levels, hidden = wr_ref.shape
    face = atoms // 8
    wide = 2 * atoms
    span = group * atoms
    f32_of = lambda rows: rows.astype(F32)
    even, odd = where_ref[0:1], where_ref[1:2]
    cross = f32_of(cross_ref[...])
    flip_faces, flip_spots = f32_of(flip_ref[: 2 * face]), f32_of(flip_ref[2 * atoms :])
    below = odd * flip_faces + even * cross[: 2 * face]
    above = even * flip_faces + odd * cross[: 2 * face]
    ghosts = (
        (below[face:], odd * flip_spots + even * cross[2 * face :], 1),
        (above[:face], even * flip_spots + odd * cross[2 * face :], 0),
        (f32_of(below_ref[3 * face : 4 * face]), f32_of(below_ref[2 * atoms :]), 3),
        (f32_of(above_ref[2 * face : 3 * face]), f32_of(above_ref[2 * atoms :]), 2),
    )
    lane = lax.broadcasted_iota(jnp.int32, (POS_ROWS, atoms), 1)
    ghost = jnp.zeros((POS_ROWS, atoms), F32)
    for slot, (_, spot, source) in enumerate(ghosts):
        turned = pltpu.roll(spot, ((slot - source) * face) % atoms, 1)
        inside = (lane >= slot * face) & (lane < (slot + 1) * face)
        ghost = jnp.where(inside, turned, ghost)
    own_rows = own_ref[2 * atoms :]
    places = jnp.concatenate([own_rows, ghost.astype(BF16)], axis=1)
    rows = [f32_of(own_ref[:atoms])] + [g[0] for g in ghosts]
    rows.append(jnp.zeros((wide - atoms - 4 * face, channels), F32))
    features_t = jnp.concatenate(rows, axis=0).T.astype(BF16)
    mat_ref[:channels, :] = features_t
    mat_ref[channels:, :] = places
    cot_t = f32_of(own_ref[atoms : 2 * atoms]).T * (1.0 / math.sqrt(slots))
    source_pos = pos_of(own_rows)
    source_pos = jnp.concatenate([source_pos] * group, axis=1)
    cot_rep = jnp.concatenate([cot_t] * group, axis=1)
    steps = lax.broadcasted_iota(jnp.int32, (levels, span), 0).astype(F32)
    rates = 0.5 * jnp.exp(steps * (math.log(16.0) / (levels - 1)))
    buffer_row = lax.broadcasted_iota(jnp.int32, (wide, span), 0)
    axis = lax.broadcasted_iota(jnp.int32, (8, span), 0)
    w_radial = wr_ref[...]
    w_out = wo_ref[...]
    buf_acc[...] = jnp.zeros_like(buf_acc)
    grad_out[...] = jnp.zeros_like(grad_out)
    move_out[...] = jnp.zeros_like(move_out)

    def step(g, carry):
        index = jnp.concatenate([nbr_ref[pl.ds(g * group + s, 1), :] for s in range(group)], axis=1)
        live = jnp.concatenate(
            [jnp.where(count_ref[...] > g * group + s, 1.0, 0.0) for s in range(group)], axis=1
        )
        picked = jnp.where(buffer_row == index, 1.0, 0.0).astype(BF16)
        taken = mm(mat_ref[...], picked, NN)
        feat = taken[:channels]
        offset = jnp.where(axis < 3, pos_of(taken[channels:]) - source_pos, 0.0)
        cosine, chord = turn_trig(offset)
        dist2 = jnp.sum(chord * chord, axis=0, keepdims=True)
        rbf = jnp.exp(-rates * dist2)
        rbf_h = rbf.astype(BF16)
        pre = mm(w_radial, rbf_h, TN)
        gate = jax.nn.sigmoid(pre)
        act = (pre * gate).astype(BF16)
        phi = mm(w_out, act, TN)
        weight = cot_rep * live
        message = weight * phi
        high = message.astype(BF16)
        low = (message - high.astype(F32)).astype(BF16)
        buf_acc[...] += mm(picked, high, NT) + mm(picked, low, NT)
        dphi = (weight * feat).astype(BF16)
        grad_out[levels:, :] += mm(act, dphi, NT)
        d_act = mm(w_out, dphi, NN)
        dpre = (d_act * gate * (1.0 + pre * (1.0 - gate))).astype(BF16)
        grad_out[:levels, :] += mm(rbf_h, dpre, NT)
        d_rbf = mm(w_radial, dpre, NN)
        d_chord2 = -jnp.sum(d_rbf * rates * rbf, axis=0, keepdims=True)
        dmove = (2.0 * pos_unit) * d_chord2 * chord * cosine
        pieces = jnp.concatenate([v.astype(F32) for v in three_pieces(dmove)], axis=0).astype(BF16)
        moved = mm(pieces, picked, NT)
        move_out[...] += moved[0:8] + moved[8:16] + moved[16:24]
        back = dmove[:, :atoms]
        for s in range(1, group):
            back = back + dmove[:, s * atoms : (s + 1) * atoms]
        move_out[:, :atoms] -= back
        return carry

    lax.fori_loop(0, slots // group, step, 0)
    buf_out[...] = buf_acc[: atoms + 4 * face]
    extra = extra_ref.shape[0]
    for j in range(3):
        part = grad_out[j * extra : min((j + 1) * extra, levels + hidden)]
        extra_ref[: part.shape[0], j * channels : (j + 1) * channels] = part.astype(BF16)
    places = jnp.concatenate([f32_of(v) for v in packed(move_out[:, atoms:])], axis=0)
    group_0, group_1 = buf_acc[atoms : atoms + face], buf_acc[atoms + face : atoms + 2 * face]
    extra_ref[:face, 3 * channels :] = (even * group_0 + odd * group_1).astype(BF16)
    extra_ref[face : face + 16, 3 * channels :] = places.astype(BF16)


def pair_part(where, sources, neighbours, counts, w_radial, w_out, pos_unit):
    _, atoms = neighbours.shape
    levels, hidden = w_radial.shape
    channels = w_out.shape[1]
    face = atoms // 8
    group = GROUP
    return pl.pallas_call(
        functools.partial(pair_body, atoms, channels, group, pos_unit),
        out_shape=(
            jax.ShapeDtypeStruct((atoms + 4 * face, channels), F32),
            jax.ShapeDtypeStruct((8, 2 * atoms), F32),
            jax.ShapeDtypeStruct((levels + hidden, channels), F32),
            jax.ShapeDtypeStruct((extra_rows(levels + hidden, face), 4 * channels), BF16),
        ),
        scratch_shapes=[
            pltpu.VMEM((2 * atoms, channels), F32),
            pltpu.VMEM((channels + POS_ROWS, 2 * atoms), BF16),
        ],
        compiler_params=pltpu.CompilerParams(vmem_limit_bytes=12 * 2**20),
        cost_estimate=pl.CostEstimate(
            flops=4_000_000_000, bytes_accessed=1_000_000, transcendentals=500_000
        ),
        name="pairs",
    )(where, *sources, neighbours, counts.reshape(1, atoms), w_radial, w_out)


def finish_body(atoms, n_msg, scale, own_ref, total_ref, *refs):
    msgs, (feat_ref, pos_ref, filter_ref, radial_ref, out_ref) = refs[:n_msg], refs[n_msg:]
    feat, place, grad = own_ref[:atoms], own_ref[atoms : atoms + 8], own_ref[atoms + 8 :]
    for m in msgs:
        feat = feat + m[:atoms].astype(F32)
        place = place + pos_of(m[atoms : atoms + POS_ROWS])
        grad = grad + m[atoms + POS_ROWS :].astype(F32)
    levels = radial_ref.shape[0]
    c = feat_ref.shape[1]
    re = total_ref[:, :c] * total_ref[:, c : 2 * c]
    filter_ref[...] = re + total_ref[:, 2 * c : 3 * c] * total_ref[:, 3 * c :]
    feat_ref[...] = feat
    pos_ref[...] = place[0:3]
    radial_ref[...] = scale * grad[:levels]
    out_ref[...] = scale * grad[levels:]


def finish(scale, atoms, levels, own, total, msgs):
    channels = own.shape[1]
    return pl.pallas_call(
        functools.partial(finish_body, atoms, len(msgs), scale),
        out_shape=(
            jax.ShapeDtypeStruct((atoms, channels), F32),
            jax.ShapeDtypeStruct((3, atoms), F32),
            jax.ShapeDtypeStruct((total.shape[0], channels), F32),
            jax.ShapeDtypeStruct((levels, channels), F32),
            jax.ShapeDtypeStruct((own.shape[0] - atoms - 8 - levels, channels), F32),
        ),
        compiler_params=pltpu.CompilerParams(vmem_limit_bytes=8 * 2**20),
        name="finish",
    )(own, total, *msgs)


def along(block, axis, shift):
    n = lax.axis_size(axis)
    return lax.ppermute(block, axis, [((i - shift) % n, i) for i in range(n)])


def swapped(block, axis, mask):
    n = lax.axis_size(axis)
    return lax.ppermute(block, axis, [(i, i ^ mask) for i in range(n)])


def bits_of(n):
    return [1 << b for b in range(n.bit_length() - 1)]


def reordered(values, index, axis):
    n = values.shape[axis]
    for bit in bits_of(n):
        shape = values.shape[:axis] + (n // (2 * bit), 2, bit) + values.shape[axis + 1 :]
        split = values.reshape(shape)
        turned = jnp.flip(split, axis + 1)
        values = jnp.where((index & bit) > 0, turned, split).reshape(values.shape)
    return values


def program(features, cotangent, positions, neighbours, counts, k_index, k_filter, w_radial, w_out):
    atoms, channels = features.shape
    n_dom, n_slab = lax.axis_size("dom"), lax.axis_size("slab")
    devices = n_dom * n_slab
    chips = n_dom // 2
    scale = 1.0 / math.sqrt(atoms * devices)
    k_total = k_index.shape[1]
    pos_unit = 1.0 / math.sqrt(k_total)
    block = k_total // devices
    dom, slab = lax.axis_index("dom"), lax.axis_index("slab")

    own, faces = pack(features, cotangent, positions)
    msgs = [own]
    for d in range(1, n_slab):
        msgs.append(along(own, "slab", d))
    across = [(i, (i + 1 if i % 2 else i - 1) % n_dom) for i in range(n_dom)]
    cross = lax.ppermute(faces, "dom", across)
    others = [swapped(own, "dom", 1)]

    core, chip = dom & 1, dom >> 1
    k_own = k_index.reshape(3, chips, 2 * n_slab, block)
    k_own = lax.dynamic_index_in_dim(k_own, core * n_slab + slab, 2, False)
    k_own = reordered(k_own, chip, 1).reshape(3, chips * block)
    k_own = k_own.astype(BF16)
    gap = jnp.zeros((5, chips * block), BF16)
    k_rows = jnp.concatenate([k_own, k_own, gap[:2], k_own, gap], axis=0)
    filter_rows = lax.dynamic_slice_in_dim(k_filter, (dom * n_slab + slab) * block, block, 0)
    across_of = ((dom ^ 1) + jnp.where(core == 0, 1, n_dom - 1)) % n_dom
    row = lax.broadcasted_iota(jnp.int32, (-(-(2 + chips) // 8) * 8, channels), 0)
    where = ((row == core) | (row == 2 + ((across_of >> 1) ^ chip))).astype(F32)
    own, k_rows, filter_rows, where = lax.optimization_barrier(
        (own, k_rows, filter_rows, where)
    )
    msgs[0] = own

    far = n_slab // 2
    near = [d for d in range(1, n_slab) if d != far]
    cos_e, sin_e, sums = structure(k_rows, (own, others[0]), atoms, channels)
    tables = {0: (cos_e, sin_e)}
    others = others + [None] * (n_slab - 1)
    for d in near:
        msgs[d], sums = lax.optimization_barrier((msgs[d], sums))
        others[d] = swapped(msgs[d], "dom", 1)
    if near:
        taken = [msgs[d] for d in near] + [others[d] for d in near]
        cos_n, sin_n, sums = structure(k_rows, taken, atoms, channels, *sums)
        for i, d in enumerate(near):
            both = (i, i + len(near))
            tables[d] = tuple([table[j] for j in both] for table in (cos_n, sin_n))
    others[far] = swapped(msgs[far], "dom", 1)
    cos_l, sin_l, sums = structure(
        k_rows, (msgs[far], others[far]), atoms, channels, *sums, chips=chips
    )
    tables[far] = (cos_l, sin_l)
    tables_own, tables_other = (
        [tables[d][part][core_of] for part in range(2) for d in range(n_slab)]
        for core_of in range(2)
    )
    s_own, *pieces = sums
    arrived = [swapped(piece, "dom", 2 * s) for s, piece in enumerate(pieces, 1)]

    cross, pieces = lax.optimization_barrier((cross, pieces))
    sources = (msgs[0], others[0], cross, msgs[1], msgs[-1])
    buf, moves, grads, riders = pair_part(
        where, sources, neighbours, counts, w_radial, w_out, pos_unit
    )
    total, share = make_shares(scale, s_own, filter_rows, riders, arrived)
    shares = [share] + [swapped(share, "dom", 2 * s) for s in range(1, chips)]

    extra = share.shape[0] - block
    settings = (atoms, n_slab, len(shares), pos_unit, extra)
    rows = n_slab * (atoms + 8)
    there = back_call(
        functools.partial(back_other_body, *settings),
        jax.ShapeDtypeStruct((rows + grads.shape[0], channels), F32),
        where,
        k_rows,
        *tables_other,
        *others,
        *shares,
        buf,
        moves,
        grads,
    )
    sent = swapped(there, "dom", 1)
    here = back_call(
        functools.partial(back_own_body, *settings),
        jax.ShapeDtypeStruct((rows, channels), F32),
        k_rows,
        *tables_own,
        *msgs,
        *shares,
        buf,
        moves,
    )
    message = jax.ShapeDtypeStruct((atoms + POS_ROWS + grads.shape[0], channels), BF16)
    own_sum, *partials = back_call(
        functools.partial(join_body, atoms, n_slab),
        (jax.ShapeDtypeStruct((atoms + 8 + grads.shape[0], channels), F32),)
        + (message,) * (n_slab - 1),
        here,
        there,
        sent,
    )
    returned = [along(partials[d - 1], "slab", -d) for d in [far] + near]
    return finish(scale, atoms, w_radial.shape[0], own_sum, total, returned)


def solution(mesh):
    in_specs = (
        P(("dom", "slab"), None),
        P(("dom", "slab"), None),
        P(None, ("dom", "slab")),
        P(None, ("dom", "slab")),
        P(("dom", "slab")),
        P(),
        P(),
        P(),
        P(),
    )
    out_specs = (
        P(("dom", "slab"), None),
        P(None, ("dom", "slab")),
        P(("dom", "slab"), None),
        P(),
        P(),
    )
    return jax.shard_map(program, mesh=mesh, in_specs=in_specs, out_specs=out_specs, check_vma=False)
```

```python
import functools
import math

import jax
import jax.numpy as jnp
from jax import lax
from jax.experimental import pallas as pl
from jax.experimental.pallas import tpu as pltpu
from jax.sharding import PartitionSpec as P


F32 = jnp.float32
BF16 = jnp.bfloat16
GROUP = 16
POS_ROWS = 16
MAGIC = 12582912.0
SIN_POLY = (
    6.28318528028833,
    -10.335420168095697,
    5.100155056857644,
    -1.196582599540606,
    0.15531532235506335,
)
COS_POLY = (
    0.9999999532943689,
    -4.934792832496617,
    4.058411371007551,
    -1.331876617475819,
    0.21968961468319229,
)


def horner(coefs, w):
    acc = jnp.full_like(w, coefs[-1])
    for c in coefs[-2::-1]:
        acc = acc * w + c
    return acc


def turn_trig(t):
    u = t - ((t + MAGIC) - MAGIC)
    w = u * u
    twice_sin = u * horner(SIN_POLY, w)
    half_cos = horner(COS_POLY, w)
    return 1.0 - 0.5 * twice_sin * twice_sin, twice_sin * half_cos


def three_pieces(value):
    high = value.astype(BF16)
    rest = value - high.astype(F32)
    mid = rest.astype(BF16)
    low = (rest - mid.astype(F32)).astype(BF16)
    return high, mid, low


def mm(first, second, dims):
    return lax.dot_general(first, second, (dims, ((), ())), preferred_element_type=F32)


NN = ((1,), (0,))
TN = ((0,), (0,))
NT = ((1,), (1,))


def packed(value):
    high, mid, low = (piece.astype(F32) for piece in three_pieces(value))
    return (high + pltpu.roll(mid, 3, 0)).astype(BF16), low.astype(BF16)


def place_rows(positions):
    zeros = jnp.zeros((5, positions.shape[1]), F32)
    first, second = packed(jnp.concatenate([positions, zeros], axis=0))
    return jnp.concatenate([first.astype(F32), second.astype(F32)], axis=0).astype(BF16)


def pos_of(rows, pieces=3):
    rows = rows.astype(F32)
    total = rows[0:8] + pltpu.roll(rows[0:8], 5, 0)
    return total + rows[8:16] if pieces == 3 else total


def pack_body(feat_hbm, cot_hbm, pos_hbm, own_ref, face_ref, pos_ref, sems):
    atoms = feat_hbm.shape[0]
    faces = 2 * (atoms // 8)
    copies = [
        pltpu.make_async_copy(pos_hbm, pos_ref, sems.at[0]),
        pltpu.make_async_copy(feat_hbm, own_ref.at[pl.ds(0, atoms)], sems.at[1]),
        pltpu.make_async_copy(cot_hbm, own_ref.at[pl.ds(atoms, atoms)], sems.at[2]),
    ]
    for copy in copies:
        copy.start()
    copies[0].wait()
    places = place_rows(pos_ref[...])
    own_ref[2 * atoms :, :] = places
    face_ref[faces:, :] = places
    copies[1].wait()
    face_ref[:faces, :] = own_ref[:faces]
    copies[2].wait()


def pack(features, cotangent, positions):
    atoms, channels = features.shape
    return pl.pallas_call(
        pack_body,
        out_shape=(
            jax.ShapeDtypeStruct((2 * atoms + POS_ROWS, channels), BF16),
            jax.ShapeDtypeStruct((2 * (atoms // 8) + POS_ROWS, channels), BF16),
        ),
        in_specs=[pl.BlockSpec(memory_space=pl.ANY)] * 3,
        scratch_shapes=[pltpu.VMEM((3, atoms), F32), pltpu.SemaphoreType.DMA((3,))],
        name="pack",
    )(features, cotangent, positions)


def structure_body(atoms, n_msg, has_partial, block, k_ref, *refs):
    msgs, refs = refs[:n_msg], refs[n_msg:]
    partial, refs = (refs[0], refs[1:]) if has_partial else (None, refs)
    cos_refs, sin_refs, out_refs = refs[:n_msg], refs[n_msg : 2 * n_msg], refs[2 * n_msg :]
    k_total = k_ref.shape[1]
    places = jnp.concatenate([m[2 * atoms :] for m in msgs], axis=1)
    values = jnp.concatenate(
        [jnp.concatenate([m[:atoms], m[atoms : 2 * atoms]], axis=1) for m in msgs], axis=0
    )
    rows = min(128, k_total)
    for j in range(k_total // rows):
        span = slice(j * rows, (j + 1) * rows)
        cosine, sine = turn_trig(mm(k_ref[:, span], places, TN))
        for i, (cos_ref, sin_ref) in enumerate(zip(cos_refs, sin_refs)):
            cos_ref[span, :] = cosine[:, i * atoms : (i + 1) * atoms]
            sin_ref[span, :] = sine[:, i * atoms : (i + 1) * atoms]
        re, im = mm(cosine.astype(BF16), values, NN), mm(sine.astype(BF16), values, NN)
        width = re.shape[1]
        if has_partial:
            re = re + partial[span, :width]
            im = im + partial[span, width:]
        if len(out_refs) == 1:
            out_refs[0][span, :width] = re
            out_refs[0][span, width:] = im
            continue
        for at in range(span.start // block, span.stop // block):
            part = slice(at * block - span.start, (at + 1) * block - span.start)
            out_refs[at][:, :width] = re[part].astype(out_refs[at].dtype)
            out_refs[at][:, width:] = im[part].astype(out_refs[at].dtype)


def structure(k_rows, msgs, atoms, channels, partial=None, chips=1):
    k_total = k_rows.shape[1]
    n = len(msgs)
    block = k_total // chips
    tables = (jax.ShapeDtypeStruct((k_total, atoms), F32),) * (2 * n)
    sums = (jax.ShapeDtypeStruct((block, 4 * channels), F32),)
    sums += (jax.ShapeDtypeStruct((block, 4 * channels), BF16),) * (chips - 1)
    operands = (k_rows, *msgs) + (() if partial is None else (partial,))
    outs = pl.pallas_call(
        functools.partial(structure_body, atoms, n, partial is not None, block),
        out_shape=tables + sums,
        compiler_params=pltpu.CompilerParams(vmem_limit_bytes=8 * 2**20),
        cost_estimate=pl.CostEstimate(
            flops=1_000_000_000 * n, bytes_accessed=1_000_000 * n, transcendentals=0
        ),
    )(*operands)
    return outs[:n], outs[n : 2 * n], outs[2 * n :]


def extra_rows(grad_rows, face):
    return -(-max(-(-grad_rows // 3), face + 16) // 16) * 16


def shares_body(scale, own_ref, filter_ref, extra_ref, *refs):
    others, (total_ref, share_ref) = refs[:-2], refs[-2:]
    total = own_ref[...]
    for other in others:
        total = total + other[...].astype(F32)
    total = scale * total
    total_ref[...] = total
    extra = extra_ref.shape[0]
    share_ref[:extra, :] = extra_ref[...]
    share_ref[extra:, :] = (jnp.concatenate([filter_ref[...]] * 4, axis=1) * total).astype(BF16)


def make_shares(scale, own, k_filter, extra, others):
    return pl.pallas_call(
        functools.partial(shares_body, scale),
        out_shape=(
            jax.ShapeDtypeStruct(own.shape, F32),
            jax.ShapeDtypeStruct((extra.shape[0] + own.shape[0], own.shape[1]), BF16),
        ),
        compiler_params=pltpu.CompilerParams(vmem_limit_bytes=8 * 2**20),
        cost_estimate=pl.CostEstimate(
            flops=200_000_000, bytes_accessed=600_000, transcendentals=0
        ),
        name="shares",
    )(own, k_filter, extra, *others)


def half_backward(atoms, pos_unit, msgs, k_ref, cos_refs, sin_refs, shares, extra):
    c = shares[0].shape[1] // 4
    share = jnp.concatenate([s[extra:] for s in shares], axis=0)
    source = jnp.concatenate(
        [
            jnp.concatenate([m[atoms : 2 * atoms], m[:atoms]], axis=1)
            for m in (ref[...] for ref in msgs)
        ],
        axis=0,
    )
    cosine = jnp.concatenate([ref[...] for ref in cos_refs], axis=1)
    sine = jnp.concatenate([ref[...] for ref in sin_refs], axis=1)
    feat = mm(share[:, c : 2 * c], cosine.astype(BF16), TN) + mm(
        share[:, 3 * c :], sine.astype(BF16), TN
    )
    p = mm(share[:, : 2 * c], source, NT)
    q = mm(share[:, 2 * c :], source, NT)
    weight = cosine * q - sine * p
    high = weight.astype(BF16)
    low = (weight - high.astype(F32)).astype(BF16)
    k16 = k_ref[...]
    place = (mm(k16, high, NN) + mm(k16, low, NN))[0:8]
    row = lax.broadcasted_iota(jnp.int32, place.shape, 0)
    return feat, jnp.where(row < 3, pos_unit * place, 0.0)


def group_rows(value, face, atoms, group):
    c = value.shape[1]
    above, below = group * face, atoms - (group + 1) * face
    pieces = [jnp.zeros((above, c), F32)] if above else []
    return jnp.concatenate(pieces + [value, jnp.zeros((below, c), F32)], axis=0)


def group_lanes(value, face, source, group):
    atoms = value.shape[1]
    lane = lax.broadcasted_iota(jnp.int32, value.shape, 1)
    turned = pltpu.roll(value, ((group - source) * face) % atoms, 1)
    return jnp.where((lane >= group * face) & (lane < (group + 1) * face), turned, 0.0)


def back_other_body(atoms, n_msg, n_share, pos_unit, extra, where_ref, k_ref, *refs):
    cos_refs, sin_refs, msgs = refs[:n_msg], refs[n_msg : 2 * n_msg], refs[2 * n_msg : 3 * n_msg]
    refs = refs[3 * n_msg :]
    shares, refs = refs[:n_share], refs[n_share:]
    buf_ref, move_ref, grad0_ref, sum_ref = refs
    c = buf_ref.shape[1]
    face = atoms // 8
    grad = grad0_ref[...]
    passed = jnp.zeros((face, c), F32)
    passed_moves = jnp.zeros((8, atoms), F32)
    for j, ref in enumerate(shares):
        if j:
            parts = [ref[:extra, i * c : (i + 1) * c].astype(F32) for i in range(3)]
            grad = grad + jnp.concatenate(parts, axis=0)[: grad.shape[0]]
        backs = ref[: face + 16, 3 * c :].astype(F32)
        sel = where_ref[2 + j : 3 + j]
        passed = passed + sel * backs[:face]
        tile = backs[face : face + 8]
        passed_moves = passed_moves + sel * (tile + pltpu.roll(tile, 5, 0) + backs[face + 8 :])
    even, odd = where_ref[0:1], where_ref[1:2]
    ghost_0, ghost_1 = buf_ref[atoms : atoms + face], buf_ref[atoms + face : atoms + 2 * face]
    rows_0 = even * ghost_1 + odd * passed
    rows_1 = even * passed + odd * ghost_0
    ours = move_ref[:, atoms:]
    moves = group_lanes(even * ours + odd * passed_moves, face, 1, 0) + group_lanes(
        even * passed_moves + odd * ours, face, 0, 1
    )
    feat, place = half_backward(
        atoms, pos_unit, msgs, k_ref, cos_refs, sin_refs, shares, extra
    )
    for d in range(n_msg):
        rows = feat[:, d * atoms : (d + 1) * atoms].T
        spots = place[:, d * atoms : (d + 1) * atoms]
        if d == 0:
            top = jnp.concatenate([rows_0, rows_1], axis=0)
            rows = jnp.concatenate([rows[: 2 * face] + top, rows[2 * face :]], axis=0)
            spots = spots + moves
        sum_ref[d * atoms : (d + 1) * atoms, :] = rows
        first = n_msg * atoms + d * 8
        sum_ref[first : first + 8, :] = spots
    sum_ref[n_msg * (atoms + 8) :, :] = grad


def back_own_body(atoms, n_msg, n_share, pos_unit, extra, k_ref, *refs):
    cos_refs, sin_refs, msgs = refs[:n_msg], refs[n_msg : 2 * n_msg], refs[2 * n_msg : 3 * n_msg]
    refs = refs[3 * n_msg :]
    shares, refs = refs[:n_share], refs[n_share:]
    buf_ref, move_ref, sum_ref = refs
    face = atoms // 8
    feat, place = half_backward(
        atoms, pos_unit, msgs, k_ref, cos_refs, sin_refs, shares, extra
    )
    ghost_move = move_ref[:, atoms:]
    for d in range(n_msg):
        rows = feat[:, d * atoms : (d + 1) * atoms].T
        spots = place[:, d * atoms : (d + 1) * atoms]
        if d == 0:
            rows = rows + buf_ref[:atoms]
            spots = spots + move_ref[:, :atoms]
        for shift, ghost, group in ((1, 2, 3), (n_msg - 1, 3, 2)):
            if d == shift:
                part = buf_ref[atoms + ghost * face : atoms + (ghost + 1) * face]
                rows = rows + group_rows(part, face, atoms, group)
                spots = spots + group_lanes(ghost_move, face, ghost, group)
        sum_ref[d * atoms : (d + 1) * atoms, :] = rows
        first = n_msg * atoms + d * 8
        sum_ref[first : first + 8, :] = spots


def join_body(atoms, n_msg, here_ref, there_ref, sent_ref, own_ref, *out_refs):
    tail = n_msg * (atoms + 8)
    row = lax.broadcasted_iota(jnp.int32, (8, atoms), 0)
    grad = sent_ref[tail:] + there_ref[tail:]
    own_ref[atoms + 8 :, :] = grad
    grad = grad.astype(BF16)
    for d in range(n_msg):
        span = slice(d * atoms, (d + 1) * atoms)
        spot = slice(n_msg * atoms + d * 8, n_msg * atoms + d * 8 + 8)
        rows = here_ref[span] + sent_ref[span]
        spots = here_ref[spot] + sent_ref[spot]
        if d == 0:
            own_ref[:atoms, :] = rows
            own_ref[atoms : atoms + 8, :] = spots
            continue
        out = out_refs[d - 1]
        out[:atoms, :] = rows.astype(BF16)
        spots = jnp.where(row < 3, spots, 0.0)
        out[atoms : atoms + grad.shape[0], :] = grad
        out[atoms + grad.shape[0] :, :] = packed(spots)[0]


def back_call(body, out_shape, *operands):
    return pl.pallas_call(
        body,
        out_shape=out_shape,
        compiler_params=pltpu.CompilerParams(vmem_limit_bytes=8 * 2**20),
        cost_estimate=pl.CostEstimate(
            flops=3_000_000_000, bytes_accessed=4_000_000, transcendentals=0
        ),
    )(*operands)


def pair_body(
    atoms,
    channels,
    group,
    pos_unit,
    where_ref,
    own_ref,
    flip_ref,
    cross_ref,
    below_ref,
    above_ref,
    nbr_ref,
    count_ref,
    wr_ref,
    wo_ref,
    buf_out,
    move_out,
    grad_out,
    extra_ref,
    buf_acc,
    mat_ref,
):
    slots = nbr_ref.shape[0]
    levels, hidden = wr_ref.shape
    face = atoms // 8
    wide = 2 * atoms
    span = group * atoms
    f32_of = lambda rows: rows.astype(F32)
    even, odd = where_ref[0:1], where_ref[1:2]
    cross = f32_of(cross_ref[...])
    flip_faces, flip_spots = f32_of(flip_ref[: 2 * face]), f32_of(flip_ref[2 * atoms :])
    below = odd * flip_faces + even * cross[: 2 * face]
    above = even * flip_faces + odd * cross[: 2 * face]
    ghosts = (
        (below[face:], odd * flip_spots + even * cross[2 * face :], 1),
        (above[:face], even * flip_spots + odd * cross[2 * face :], 0),
        (f32_of(below_ref[3 * face : 4 * face]), f32_of(below_ref[2 * atoms :]), 3),
        (f32_of(above_ref[2 * face : 3 * face]), f32_of(above_ref[2 * atoms :]), 2),
    )
    lane = lax.broadcasted_iota(jnp.int32, (POS_ROWS, atoms), 1)
    ghost = jnp.zeros((POS_ROWS, atoms), F32)
    for slot, (_, spot, source) in enumerate(ghosts):
        turned = pltpu.roll(spot, ((slot - source) * face) % atoms, 1)
        inside = (lane >= slot * face) & (lane < (slot + 1) * face)
        ghost = jnp.where(inside, turned, ghost)
    own_rows = own_ref[2 * atoms :]
    places = jnp.concatenate([own_rows, ghost.astype(BF16)], axis=1)
    rows = [f32_of(own_ref[:atoms])] + [g[0] for g in ghosts]
    rows.append(jnp.zeros((wide - atoms - 4 * face, channels), F32))
    features_t = jnp.concatenate(rows, axis=0).T.astype(BF16)
    mat_ref[:channels, :] = features_t
    mat_ref[channels:, :] = places
    cot_t = f32_of(own_ref[atoms : 2 * atoms]).T * (1.0 / math.sqrt(slots))
    source_pos = pos_of(own_rows)
    source_pos = jnp.concatenate([source_pos] * group, axis=1)
    cot_rep = jnp.concatenate([cot_t] * group, axis=1)
    steps = lax.broadcasted_iota(jnp.int32, (levels, span), 0).astype(F32)
    rates = 0.5 * jnp.exp(steps * (math.log(16.0) / (levels - 1)))
    buffer_row = lax.broadcasted_iota(jnp.int32, (wide, span), 0)
    axis = lax.broadcasted_iota(jnp.int32, (8, span), 0)
    w_radial = wr_ref[...]
    w_out = wo_ref[...]
    buf_acc[...] = jnp.zeros_like(buf_acc)
    grad_out[...] = jnp.zeros_like(grad_out)
    move_out[...] = jnp.zeros_like(move_out)

    def step(g, carry):
        index = jnp.concatenate([nbr_ref[pl.ds(g * group + s, 1), :] for s in range(group)], axis=1)
        live = jnp.concatenate(
            [jnp.where(count_ref[...] > g * group + s, 1.0, 0.0) for s in range(group)], axis=1
        )
        picked = jnp.where(buffer_row == index, 1.0, 0.0).astype(BF16)
        taken = mm(mat_ref[...], picked, NN)
        feat = taken[:channels]
        offset = jnp.where(axis < 3, pos_of(taken[channels:]) - source_pos, 0.0)
        cosine, chord = turn_trig(offset)
        dist2 = jnp.sum(chord * chord, axis=0, keepdims=True)
        rbf = jnp.exp(-rates * dist2)
        rbf_h = rbf.astype(BF16)
        pre = mm(w_radial, rbf_h, TN)
        gate = jax.nn.sigmoid(pre)
        act = (pre * gate).astype(BF16)
        phi = mm(w_out, act, TN)
        weight = cot_rep * live
        message = weight * phi
        high = message.astype(BF16)
        low = (message - high.astype(F32)).astype(BF16)
        buf_acc[...] += mm(picked, high, NT) + mm(picked, low, NT)
        dphi = (weight * feat).astype(BF16)
        grad_out[levels:, :] += mm(act, dphi, NT)
        d_act = mm(w_out, dphi, NN)
        dpre = (d_act * gate * (1.0 + pre * (1.0 - gate))).astype(BF16)
        grad_out[:levels, :] += mm(rbf_h, dpre, NT)
        d_rbf = mm(w_radial, dpre, NN)
        d_chord2 = -jnp.sum(d_rbf * rates * rbf, axis=0, keepdims=True)
        dmove = (2.0 * pos_unit) * d_chord2 * chord * cosine
        pieces = jnp.concatenate([v.astype(F32) for v in three_pieces(dmove)], axis=0).astype(BF16)
        moved = mm(pieces, picked, NT)
        move_out[...] += moved[0:8] + moved[8:16] + moved[16:24]
        back = dmove[:, :atoms]
        for s in range(1, group):
            back = back + dmove[:, s * atoms : (s + 1) * atoms]
        move_out[:, :atoms] -= back
        return carry

    lax.fori_loop(0, slots // group, step, 0)
    buf_out[...] = buf_acc[: atoms + 4 * face]
    extra = extra_ref.shape[0]
    for j in range(3):
        part = grad_out[j * extra : min((j + 1) * extra, levels + hidden)]
        extra_ref[: part.shape[0], j * channels : (j + 1) * channels] = part.astype(BF16)
    places = jnp.concatenate([f32_of(v) for v in packed(move_out[:, atoms:])], axis=0)
    group_0, group_1 = buf_acc[atoms : atoms + face], buf_acc[atoms + face : atoms + 2 * face]
    extra_ref[:face, 3 * channels :] = (even * group_0 + odd * group_1).astype(BF16)
    extra_ref[face : face + 16, 3 * channels :] = places.astype(BF16)


def pair_part(where, sources, neighbours, counts, w_radial, w_out, pos_unit):
    _, atoms = neighbours.shape
    levels, hidden = w_radial.shape
    channels = w_out.shape[1]
    face = atoms // 8
    group = GROUP
    return pl.pallas_call(
        functools.partial(pair_body, atoms, channels, group, pos_unit),
        out_shape=(
            jax.ShapeDtypeStruct((atoms + 4 * face, channels), F32),
            jax.ShapeDtypeStruct((8, 2 * atoms), F32),
            jax.ShapeDtypeStruct((levels + hidden, channels), F32),
            jax.ShapeDtypeStruct((extra_rows(levels + hidden, face), 4 * channels), BF16),
        ),
        scratch_shapes=[
            pltpu.VMEM((2 * atoms, channels), F32),
            pltpu.VMEM((channels + POS_ROWS, 2 * atoms), BF16),
        ],
        compiler_params=pltpu.CompilerParams(vmem_limit_bytes=12 * 2**20),
        cost_estimate=pl.CostEstimate(
            flops=4_000_000_000, bytes_accessed=1_000_000, transcendentals=500_000
        ),
        name="pairs",
    )(where, *sources, neighbours, counts.reshape(1, atoms), w_radial, w_out)


def finish_body(atoms, n_msg, scale, own_ref, total_ref, *refs):
    msgs, (feat_ref, pos_ref, filter_ref, radial_ref, out_ref) = refs[:n_msg], refs[n_msg:]
    feat, place, grad = own_ref[:atoms], own_ref[atoms : atoms + 8], own_ref[atoms + 8 :]
    for m in msgs:
        feat = feat + m[:atoms].astype(F32)
        place = place + pos_of(m[atoms + grad.shape[0] :], 2)
        grad = grad + m[atoms : atoms + grad.shape[0]].astype(F32)
    levels = radial_ref.shape[0]
    c = feat_ref.shape[1]
    re = total_ref[:, :c] * total_ref[:, c : 2 * c]
    filter_ref[...] = re + total_ref[:, 2 * c : 3 * c] * total_ref[:, 3 * c :]
    feat_ref[...] = feat
    pos_ref[...] = place[0:3]
    radial_ref[...] = scale * grad[:levels]
    out_ref[...] = scale * grad[levels:]


def finish(scale, atoms, levels, own, total, msgs):
    channels = own.shape[1]
    return pl.pallas_call(
        functools.partial(finish_body, atoms, len(msgs), scale),
        out_shape=(
            jax.ShapeDtypeStruct((atoms, channels), F32),
            jax.ShapeDtypeStruct((3, atoms), F32),
            jax.ShapeDtypeStruct((total.shape[0], channels), F32),
            jax.ShapeDtypeStruct((levels, channels), F32),
            jax.ShapeDtypeStruct((own.shape[0] - atoms - 8 - levels, channels), F32),
        ),
        compiler_params=pltpu.CompilerParams(vmem_limit_bytes=8 * 2**20),
        name="finish",
    )(own, total, *msgs)


def along(block, axis, shift):
    n = lax.axis_size(axis)
    return lax.ppermute(block, axis, [((i - shift) % n, i) for i in range(n)])


def swapped(block, axis, mask):
    n = lax.axis_size(axis)
    return lax.ppermute(block, axis, [(i, i ^ mask) for i in range(n)])


def bits_of(n):
    return [1 << b for b in range(n.bit_length() - 1)]


def reordered(values, index, axis):
    n = values.shape[axis]
    for bit in bits_of(n):
        shape = values.shape[:axis] + (n // (2 * bit), 2, bit) + values.shape[axis + 1 :]
        split = values.reshape(shape)
        turned = jnp.flip(split, axis + 1)
        values = jnp.where((index & bit) > 0, turned, split).reshape(values.shape)
    return values


def program(features, cotangent, positions, neighbours, counts, k_index, k_filter, w_radial, w_out):
    atoms, channels = features.shape
    n_dom, n_slab = lax.axis_size("dom"), lax.axis_size("slab")
    devices = n_dom * n_slab
    chips = n_dom // 2
    scale = 1.0 / math.sqrt(atoms * devices)
    k_total = k_index.shape[1]
    pos_unit = 1.0 / math.sqrt(k_total)
    block = k_total // devices
    dom, slab = lax.axis_index("dom"), lax.axis_index("slab")

    own, faces = pack(features, cotangent, positions)
    msgs = [own]
    for d in range(1, n_slab):
        msgs.append(along(own, "slab", d))
    across = [(i, (i + 1 if i % 2 else i - 1) % n_dom) for i in range(n_dom)]
    cross = lax.ppermute(faces, "dom", across)
    others = [swapped(own, "dom", 1)]

    core, chip = dom & 1, dom >> 1
    k_own = k_index.reshape(3, chips, 2 * n_slab, block)
    k_own = lax.dynamic_index_in_dim(k_own, core * n_slab + slab, 2, False)
    k_own = reordered(k_own, chip, 1).reshape(3, chips * block)
    k_own = k_own.astype(BF16)
    gap = jnp.zeros((5, chips * block), BF16)
    k_rows = jnp.concatenate([k_own, k_own, gap[:2], k_own, gap], axis=0)
    filter_rows = lax.dynamic_slice_in_dim(k_filter, (dom * n_slab + slab) * block, block, 0)
    across_of = ((dom ^ 1) + jnp.where(core == 0, 1, n_dom - 1)) % n_dom
    row = lax.broadcasted_iota(jnp.int32, (-(-(2 + chips) // 8) * 8, channels), 0)
    where = ((row == core) | (row == 2 + ((across_of >> 1) ^ chip))).astype(F32)
    own, k_rows, filter_rows, where = lax.optimization_barrier(
        (own, k_rows, filter_rows, where)
    )
    msgs[0] = own

    far = n_slab // 2
    near = [d for d in range(1, n_slab) if d != far]
    cos_e, sin_e, sums = structure(k_rows, (own, others[0]), atoms, channels)
    tables = {0: (cos_e, sin_e)}
    others = others + [None] * (n_slab - 1)
    for d in near:
        msgs[d], sums = lax.optimization_barrier((msgs[d], sums))
        others[d] = swapped(msgs[d], "dom", 1)
    if near:
        taken = [msgs[d] for d in near] + [others[d] for d in near]
        cos_n, sin_n, sums = structure(k_rows, taken, atoms, channels, *sums)
        for i, d in enumerate(near):
            both = (i, i + len(near))
            tables[d] = tuple([table[j] for j in both] for table in (cos_n, sin_n))
    others[far] = swapped(msgs[far], "dom", 1)
    cos_l, sin_l, sums = structure(
        k_rows, (msgs[far], others[far]), atoms, channels, *sums, chips=chips
    )
    tables[far] = (cos_l, sin_l)
    tables_own, tables_other = (
        [tables[d][part][core_of] for part in range(2) for d in range(n_slab)]
        for core_of in range(2)
    )
    s_own, *pieces = sums
    arrived = [swapped(piece, "dom", 2 * s) for s, piece in enumerate(pieces, 1)]

    cross, pieces = lax.optimization_barrier((cross, pieces))
    sources = (msgs[0], others[0], cross, msgs[1], msgs[-1])
    buf, moves, grads, riders = pair_part(
        where, sources, neighbours, counts, w_radial, w_out, pos_unit
    )
    total, share = make_shares(scale, s_own, filter_rows, riders, arrived)
    shares = [share] + [swapped(share, "dom", 2 * s) for s in range(1, chips)]

    extra = share.shape[0] - block
    settings = (atoms, n_slab, len(shares), pos_unit, extra)
    rows = n_slab * (atoms + 8)
    there = back_call(
        functools.partial(back_other_body, *settings),
        jax.ShapeDtypeStruct((rows + grads.shape[0], channels), F32),
        where,
        k_rows,
        *tables_other,
        *others,
        *shares,
        buf,
        moves,
        grads,
    )
    sent = swapped(there, "dom", 1)
    here = back_call(
        functools.partial(back_own_body, *settings),
        jax.ShapeDtypeStruct((rows, channels), F32),
        k_rows,
        *tables_own,
        *msgs,
        *shares,
        buf,
        moves,
    )
    message = jax.ShapeDtypeStruct((atoms + grads.shape[0] + 8, channels), BF16)
    own_sum, *partials = back_call(
        functools.partial(join_body, atoms, n_slab),
        (jax.ShapeDtypeStruct((atoms + 8 + grads.shape[0], channels), F32),)
        + (message,) * (n_slab - 1),
        here,
        there,
        sent,
    )
    returned = [along(partials[d - 1], "slab", -d) for d in [far] + near]
    return finish(scale, atoms, w_radial.shape[0], own_sum, total, returned)


def solution(mesh):
    in_specs = (
        P(("dom", "slab"), None),
        P(("dom", "slab"), None),
        P(None, ("dom", "slab")),
        P(None, ("dom", "slab")),
        P(("dom", "slab")),
        P(),
        P(),
        P(),
        P(),
    )
    out_specs = (
        P(("dom", "slab"), None),
        P(None, ("dom", "slab")),
        P(("dom", "slab"), None),
        P(),
        P(),
    )
    return jax.shard_map(program, mesh=mesh, in_specs=in_specs, out_specs=out_specs, check_vma=False)
```
